32 devices in a mesh: ens: 2 (over core), ctx: 4 (over y, x), group: 4 (over z).
Axes of the slice: x: 2, y: 2, z: 4, core: 2. Of those that a mesh axis runs over, the one named last changes fastest.
Arguments:
- latents: bfloat16 [8, 1024, 512], P('ens', ('ctx', 'group')), parts along dimension 0, may hold values from -6 to 6
- rotary_rows: bfloat16 [8, 1024, 64], P('ens', ('ctx', 'group')), parts along dimension 0, may hold values from -6 to 6
- latent_gain: float32 [512], replicated, may hold values from 0.25 to 1.75
- key_up: bfloat16 [1024, 16, 128], P('ens', 'group'), parts along dimension 0, may hold values from -0.25 to 0.25
- value_up: bfloat16 [1024, 16, 128], P('ens', 'group'), parts along dimension 0, may hold values from -0.25 to 0.25
Outputs:
- stored_keys: bfloat16 [8, 16, 192, 1024], P(('ens', 'ctx'), 'group'), parts along dimension 0
- stored_values: bfloat16 [8, 1024, 16, 128], P(('ens', 'ctx'), None, 'group'), parts along dimension 0
The draws below stay inside these ranges and needn't reach their ends.
There are 2 independent parts, one for each index of `ens`. The reference program is written for one: setup_inputs(seed, part) draws one part's arguments, and reference() takes and returns one part's arrays. A program takes and returns all parts, laid end to end along the dimension named above; an argument that names none is the same for every part. Nothing has to cross between parts.
All inputs are finite; a program needn't handle non-finite values.
Results may differ from the reference program's by a relative error of at most 0.0049.
Values may be sent and summed in bfloat16 or wider, within the bound.
A program may use at most 64 MiB of HBM per device.

```python
import jax
import jax.numpy as jnp
from jax import lax

BATCH = 4
LENGTH = 1024
HEADS = 16
LATENT = 512
KEY_PART = 128
ROTARY = 64
VALUE_SIZE = 128


def levels(key, extent, split, low, top_value):
    loudness, own = 1.0, jax.random.fold_in(key, 6)
    for axis_at, shards_of in split:
        steps = jnp.exp(jax.random.uniform(jax.random.fold_in(own, axis_at), (shards_of,), jnp.float32, low / len(split), top_value / len(split)))
        loudness = loudness * jnp.repeat(steps, extent[axis_at] // shards_of).reshape([-1 if axis == axis_at else 1 for axis in range(len(extent))])
    return loudness


def gaussian(own_key, dims, width, reach, split=(), dtype=jnp.bfloat16):
    array = jax.random.normal(own_key, dims, jnp.float32) * width
    if len(split) > 0:
        array = levels(own_key, dims, split, -0.22, 0.18) * array
    return jnp.clip(array, min=-reach, max=reach).astype(dtype)


def setup_inputs(seed: int = 0, part: int = 0) -> dict:
    arg_keys = jax.random.split(jax.random.key(seed), 6)
    own_keys = jax.random.split(jax.random.fold_in(arg_keys[5], part), 6)
    latents = gaussian(own_keys[0], (BATCH, LENGTH, LATENT), 1.0, 6.0, ((1, 16),))
    rotary_rows = gaussian(own_keys[1], (BATCH, LENGTH, ROTARY), 1.0, 6.0, ((1, 16),))
    latent_gain = jnp.clip(1.0 + 0.15 * jax.random.normal(arg_keys[2], (LATENT,), jnp.float32), 0.25, 1.75)
    key_up = gaussian(own_keys[3], (LATENT, HEADS, KEY_PART), LATENT ** -0.5, 0.25, ((1, 4),))
    value_up = gaussian(own_keys[4], (LATENT, HEADS, VALUE_SIZE), LATENT ** -0.5, 0.25, ((1, 4),))
    return dict(latents=latents, rotary_rows=rotary_rows, latent_gain=latent_gain, key_up=key_up, value_up=value_up)


def root_norm(vectors, row_gain):
    return vectors * lax.rsqrt(lax.optimization_barrier(jnp.mean(vectors * vectors, axis=-1, keepdims=True)) + 1e-06) * row_gain

def reference(latents, rotary_rows, latent_gain, key_up, value_up):
    rows_ready = root_norm(latents.astype(jnp.float32), latent_gain).astype(jnp.bfloat16)
    rows_ready = lax.optimization_barrier(rows_ready)

    def expand_one(one):
        rows_one, rotary_one = one
        wide_keys = jnp.einsum('tr,rhk->thk', rows_one.astype(jnp.float32), key_up.astype(jnp.float32)).astype(jnp.bfloat16)
        shared = jnp.broadcast_to(rotary_one[:, None], (LENGTH, HEADS, ROTARY))
        wide_values = jnp.einsum('tr,rhk->thk', rows_one.astype(jnp.float32), value_up.astype(jnp.float32)).astype(jnp.bfloat16)
        return (jnp.concatenate([wide_keys, shared], axis=-1), wide_values)
    stored_keys, stored_values = lax.map(expand_one, (rows_ready, rotary_rows))
    stored_keys = jnp.transpose(stored_keys, (0, 2, 3, 1))
    return (stored_keys, stored_values)
```

```python
import functools

import jax
import jax.numpy as jnp
from jax import lax
from jax.experimental import pallas as pl
from jax.experimental.pallas import tpu as pltpu
from jax.sharding import PartitionSpec as P

MESH = pl.DeviceIdType.MESH
LANES = 128
BF16 = jnp.bfloat16


def xor(me, step, count):
    total, bit = 0, 1
    while bit < count:
        total = total + bit * lax.rem(me // bit + step // bit, 2)
        bit *= 2
    return total


def partner(me, step, count):
    return lax.rem(me + step, count) if count & (count - 1) else xor(me, step, count)


def source(me, step, count):
    return lax.rem(me + count - step, count) if count & (count - 1) else xor(me, step, count)


def turn(i, count):
    return jnp.where(i == 1, count - 1, i - 1)


def pending(c, g, seqs, planes, units):
    q = source(c, turn(jnp.int32(seqs - 1), seqs), seqs) if seqs > 1 else c
    return q, jnp.where(2 * g < planes, units - 1, 0)


def expand(block, slabs, blk, per_unit, heads, rotary, gain, key_w, value_w, mixed, put_keys, put_values):
    key_part = key_w.shape[0] // heads
    size = value_w.shape[1] // heads
    x = jnp.concatenate(
        [block(k * blk, blk).astype(jnp.float32).reshape(LANES, LANES) for k in range(slabs)],
        axis=1,
    )
    mean = jnp.mean(x * x, axis=-1, keepdims=True)
    rows = (x * lax.rsqrt(mean + 1e-06) * gain[...]).astype(BF16)
    wide_keys = lax.dot_general(
        key_w[...], rows, (((1,), (1,)), ((), ())), preferred_element_type=jnp.float32
    ).astype(BF16)
    tails = block(slabs * blk, blk * rotary // LANES).astype(jnp.float32)
    pieces = []
    for j in range(per_unit):
        pieces += [tails[j][:, :rotary], pltpu.roll(tails[j], rotary, 1)[:, :rotary]]
    turned = jnp.concatenate(pieces, axis=0).T.astype(BF16)
    for h in range(heads):
        put_keys(h, wide_keys[h * key_part : (h + 1) * key_part], turned)
    wide_values = jnp.dot(rows, value_w[...], preferred_element_type=jnp.float32)
    for h in range(heads):
        mixed[pl.ds(h, LANES, stride=heads), :] = wide_values[:, h * size : (h + 1) * size]
    put_values(mixed[...].astype(BF16))


def kernel(
    seqs, planes, heads, rotary,
    lat, rot, gain_in, key_up, value_up,
    keys, values, last, key_w, value_w, gain,
    stage, raw, mid, rot_stage, key_stage, value_stage, wide, mixed,
    load_sem, got, mid_got, sent, ready,
):
    c, g = lax.axis_index("ctx"), lax.axis_index("group")
    blk, latent = lat.shape[1:]
    slabs = latent // LANES
    tail = slabs * blk
    half = blk // 2
    per_unit = LANES // blk
    units = planes // per_unit
    key_part = key_w.shape[0] // heads
    size = value_w.shape[1] // heads
    first = partner(c, seqs - 1, seqs)

    def lat_load(s, k, sem):
        return pltpu.make_async_copy(
            lat.at[s, :, pl.ds(k * LANES, LANES)],
            stage.at[s, pl.ds(k * blk, blk), :],
            load_sem.at[sem],
        )

    rot_load = pltpu.make_async_copy(rot, rot_stage, load_sem.at[0])
    for k in range(slabs):
        lat_load(first, k, 1).start()
    rot_load.start()

    @pl.loop(1, seqs)
    def _(b):
        for k in range(slabs):
            lat_load(partner(first, b, seqs), k, 2).start()

    loads = [
        pltpu.make_async_copy(key_up, key_stage, load_sem.at[3]),
        pltpu.make_async_copy(value_up, value_stage, load_sem.at[4]),
        pltpu.make_async_copy(gain_in, gain, load_sem.at[4]),
    ]
    for load in loads:
        load.start()

    barrier = pltpu.get_barrier_semaphore()
    above, below = g < planes - 1, g > 0

    @pl.when(above)
    def _():
        pl.semaphore_signal(barrier, inc=1, device_id={"group": g + 1}, device_id_type=MESH)

    @pl.loop(c + 1, seqs)
    def _(s):
        pl.semaphore_signal(barrier, inc=1, device_id={"ctx": s}, device_id_type=MESH)

    def remote(src, dst, in_sem, to):
        return pltpu.make_async_remote_copy(
            src_ref=src, dst_ref=dst, send_sem=sent, recv_sem=in_sem,
            device_id=to, device_id_type=MESH,
        )

    def out(way, i, s, part, to):
        return remote(
            stage.at[s, part], mid.at[way, 0, i - 1, part], mid_got.at[way, 0, i - 1], {"group": to}
        )

    def own_along(to):
        return remote(stage.at[c], raw.at[c, g], got.at[g, c], {"group": to})

    def own_side(s):
        return remote(stage.at[s], raw.at[c, g], got.at[g, c], {"ctx": s})

    def forward(way, i, to):
        return remote(mid.at[way, 0, i - 1], mid.at[way, 1, i - 1], mid_got.at[way, 1, i - 1], {"group": to})

    def scatter(way, far, i, p, s):
        return remote(mid.at[way, far, i - 1], raw.at[c, p], got.at[p, c], {"ctx": s})

    def relay(p, q, to):
        return remote(raw.at[q, p], raw.at[q, p], got.at[p, q], {"group": to})

    whole = pl.ds(0, stage.shape[1])
    wide_part, rot_part = pl.ds(0, tail), pl.ds(tail, half)

    def rest(way, to):
        @pl.loop(2, seqs)
        def _(i):
            out(way, i, partner(c, turn(i, seqs), seqs), whole, to).start()

    @pl.when(c + g > 0)
    def _():
        pl.semaphore_wait(barrier, c + jnp.minimum(g, 1))

    @pl.when(below)
    def _():
        pl.semaphore_signal(ready.at[0], inc=1, device_id={"group": g - 1}, device_id_type=MESH)

    @pl.loop(0, c)
    def _(s):
        pl.semaphore_signal(ready.at[1], inc=1, device_id={"ctx": s}, device_id_type=MESH)

    for k in range(slabs):
        lat_load(first, k, 1).wait()

    @pl.when(below)
    def _():
        out(1, 1, first, wide_part, g - 1).start()

    rot_load.wait()

    @pl.loop(0, seqs)
    def _(s):
        block = rot_stage[s].astype(jnp.float32)
        both = jnp.concatenate([block[:half], block[half:]], axis=1)
        stage[s, pl.ds(tail, half), :] = both.astype(BF16)

    @pl.loop(1, seqs)
    def _(b):
        for k in range(slabs):
            lat_load(partner(first, b, seqs), k, 2).wait()

    @pl.when(below)
    def _():
        out(1, 1, first, rot_part, g - 1).start()
        own_along(g - 1).start()
        rest(1, g - 1)

    @pl.when(above)
    def _():
        pl.semaphore_wait(ready.at[0], 1)
        out(0, 1, first, whole, g + 1).start()
        own_along(g + 1).start()
        rest(0, g + 1)

    @pl.when(c < seqs - 1)
    def _():
        pl.semaphore_wait(ready.at[1], seqs - 1 - c)

    @pl.loop(1, seqs)
    def _(i):
        own_side(partner(c, turn(i, seqs), seqs)).start()

    raw[c, g] = stage[c]
    loads[0].wait()
    wide[...] = key_stage[...].astype(jnp.float32)
    for h in range(heads):
        key_w[h * key_part : (h + 1) * key_part, :] = (
            wide[pl.ds(h, latent, stride=heads), :].T.astype(BF16)
        )
    loads[1].wait()
    loads[2].wait()
    wide[...] = value_stage[...].astype(jnp.float32)
    for h in range(heads):
        value_w[:, h * size : (h + 1) * size] = (
            wide[pl.ds(h, latent, stride=heads), :].astype(BF16)
        )

    low = 2 * g < planes

    def near_first(go):
        pl.when(low)(lambda: go(1))
        go(0)
        pl.when(jnp.logical_not(low))(lambda: go(1))

    def arrived(p, q):
        relay(p, q, g).wait_recv()

    def plane(way, far):
        return g - far if way == 0 else g + far

    def exists(way, far):
        return g >= far if way == 0 else g + far < planes

    def onward(way):
        return above if way == 0 else below

    def towards(way):
        return g + 1 if way == 0 else g - 1

    def along(far):
        def go(way):
            @pl.when(exists(way, far))
            def _():
                arrived(plane(way, far), c)

                @pl.when(onward(way))
                def _():
                    relay(plane(way, far), c, towards(way)).start()

        near_first(go)

    def inner(way, far):
        return g > far if way == 0 else g + far < planes - 1

    def pass_mid(far, i):
        def go(way):
            @pl.when(exists(way, far) if far == 1 else inner(way, far))
            def _():
                forward(way, i, g).wait_recv() if far == 2 else out(way, i, c, whole, g).wait_recv()
                s = partner(c, turn(i, seqs), seqs)
                scatter(way, far - 1, i, plane(way, far), s).start()
                if far == 1:
                    @pl.when(onward(way) & inner(way, 1))
                    def _():
                        forward(way, i, towards(way)).start()

        near_first(go)

    def take(far, i):
        def go(way):
            @pl.when(exists(way, far))
            def _():
                q = source(c, turn(i, seqs), seqs)
                arrived(plane(way, far), q)

                @pl.when(onward(way) & ((far > 1) | jnp.logical_not(inner(way, 1))))
                def _():
                    relay(plane(way, far), q, towards(way)).start()

        near_first(go)

    end_q, end_u = pending(c, g, seqs, planes, units)

    def settle(q, low_far, high_far):
        @pl.loop(0, units)
        def _(u):
            far = jnp.maximum(g - u * per_unit, (u + 1) * per_unit - 1 - g)
            far = jnp.maximum(far, 1)
            wanted = (far >= low_far) & (far <= high_far)

            @pl.when(wanted & ((q != end_q) | (u != end_u)))
            def _():
                begin = u * per_unit
                start = pl.multiple_of((q * planes + begin) * blk, LANES)

                def block(row, count):
                    return raw[q, pl.ds(begin, per_unit), row : row + count, :]

                def put_keys(h, wide_keys, turned):
                    keys[h, :key_part, pl.ds(start, LANES)] = wide_keys
                    keys[h, key_part:, pl.ds(start, LANES)] = turned

                def put_values(rows):
                    at = pl.multiple_of(start * heads, LANES * heads)
                    values[pl.ds(at, LANES * heads), :] = rows

                expand(
                    block, slabs, blk, per_unit, heads, rotary, gain, key_w, value_w, mixed,
                    put_keys, put_values,
                )

    @pl.loop(1, seqs)
    def _(i):
        pass_mid(1, i)

        @pl.when(i == 1)
        def _():
            along(1)

    @pl.loop(0, seqs)
    def _(i):
        @pl.when(i == 0)
        def _():
            along(2)

        @pl.when(i > 0)
        def _():
            pass_mid(2, i)
            q = source(c, turn(i, seqs), seqs)
            arrived(g, q)
            take(1, i)

        settle(jnp.where(i == 0, c, source(c, turn(i, seqs), seqs)), 1, 1)

    @pl.loop(2, max(planes, 3))
    def _(far):
        @pl.loop(0, seqs)
        def _(i):
            @pl.when((i == 0) & (far > 2))
            def _():
                along(far)

            @pl.when(i > 0)
            def _():
                take(far, i)

            settle(jnp.where(i == 0, c, source(c, turn(i, seqs), seqs)), far, far)

    last[...] = raw[end_q, pl.ds(end_u * per_unit, per_unit)]

    ups, downs = jnp.minimum(planes - 1 - g, 1), jnp.minimum(g, 1)
    total = seqs * (ups + downs) + (seqs - 1) * (1 + ups + downs)
    total = total + seqs * (g * ups + (planes - 1 - g) * downs)
    for far in (g, planes - 1 - g):
        total = total + (seqs - 1) * jnp.where(far > 2, 1, 0)

    @pl.loop(0, total)
    def _(_):
        own_along(g).wait_send()


def store(
    seqs, planes, heads, rotary, blk,
    keys, values, last, key_w, value_w, gain,
    keys_out, values_out,
    end_keys, end_values, mixed, sems,
):
    c, g = lax.axis_index("ctx"), lax.axis_index("group")
    slabs = gain.shape[1] // LANES
    per_unit = LANES // blk
    units = planes // per_unit
    key_part = key_w.shape[0] // heads
    blocks = seqs * units
    end_q, end_u = pending(c, g, seqs, planes, units)
    end = end_q * units + end_u

    def columns(b):
        return pl.ds(pl.multiple_of(b * LANES, LANES), LANES)

    def rows(b):
        return pl.ds(pl.multiple_of(b * LANES * heads, LANES * heads), LANES * heads)

    @pl.loop(1, blocks)
    def _(j):
        b = lax.rem(end + j, blocks)
        pltpu.make_async_copy(
            keys.at[:, :, columns(b)], keys_out.at[:, :, columns(b)], sems.at[0]
        ).start()
        pltpu.make_async_copy(values.at[rows(b)], values_out.at[rows(b)], sems.at[1]).start()

    def block(row, count):
        return last[:, row : row + count, :]

    def put_keys(h, wide_keys, turned):
        end_keys[h, :key_part, :] = wide_keys
        end_keys[h, key_part:, :] = turned

    def put_values(part):
        end_values[...] = part

    expand(
        block, slabs, blk, per_unit, heads, rotary, gain, key_w, value_w, mixed,
        put_keys, put_values,
    )
    pltpu.make_async_copy(end_keys, keys_out.at[:, :, columns(end)], sems.at[0]).start()
    pltpu.make_async_copy(end_values, values_out.at[rows(end)], sems.at[1]).start()
    pltpu.make_async_copy(keys, keys_out, sems.at[0]).wait()
    pltpu.make_async_copy(values, values_out, sems.at[1]).wait()


def per_device(latents, rotary_rows, latent_gain, key_up, value_up):
    seqs, planes = lax.axis_size("ctx"), lax.axis_size("group")
    _, blk, latent = latents.shape
    rotary = rotary_rows.shape[2]
    heads, key_part = key_up.shape[1:]
    size = value_up.shape[2]
    length = seqs * planes * blk
    per_unit = LANES // blk
    packed = (blk * (latent + rotary) // LANES, LANES)
    dma = pltpu.SemaphoreType.DMA
    in_hbm = functools.partial(pltpu.with_memory_space_constraint, memory_space=pltpu.HBM)
    outer = pl.BlockSpec(memory_space=pltpu.HBM)
    inside = pl.BlockSpec(memory_space=pltpu.VMEM)
    held = pl.pallas_call(
        functools.partial(kernel, seqs, planes, heads, rotary),
        out_shape=(
            pltpu.VMEM((heads, key_part + rotary, length), BF16),
            pltpu.VMEM((length * heads, size), BF16),
            pltpu.VMEM((per_unit, *packed), BF16),
            pltpu.VMEM((heads * key_part, latent), BF16),
            pltpu.VMEM((latent, heads * size), BF16),
            pltpu.VMEM((1, latent), jnp.float32),
        ),
        in_specs=[outer] * 5,
        out_specs=(inside,) * 6,
        scratch_shapes=[
            pltpu.VMEM((seqs, *packed), BF16),
            pltpu.VMEM((seqs, planes, *packed), BF16),
            pltpu.VMEM((2, 2, seqs - 1, *packed), BF16),
            pltpu.VMEM((seqs, blk, rotary), BF16),
            pltpu.VMEM((latent * heads, key_part), BF16),
            pltpu.VMEM((latent * heads, size), BF16),
            pltpu.VMEM((latent * heads, size), jnp.float32),
            pltpu.VMEM((LANES * heads, size), jnp.float32),
            dma((5,)),
            dma((planes, seqs)),
            dma((2, 2, seqs - 1)),
            dma,
            pltpu.SemaphoreType.REGULAR((2,)),
        ],
        compiler_params=pltpu.CompilerParams(
            collective_id=0, has_side_effects=True, vmem_limit_bytes=32 * 1024 * 1024
        ),
    )(
        in_hbm(latents),
        in_hbm(rotary_rows),
        in_hbm(latent_gain.reshape(1, latent)),
        in_hbm(key_up.reshape(latent * heads, key_part)),
        in_hbm(value_up.reshape(latent * heads, size)),
    )
    keys, values = pl.pallas_call(
        functools.partial(store, seqs, planes, heads, rotary, blk),
        out_shape=(
            jax.ShapeDtypeStruct((heads, key_part + rotary, length), BF16),
            jax.ShapeDtypeStruct((length * heads, size), BF16),
        ),
        in_specs=[inside] * 6,
        out_specs=(outer, outer),
        scratch_shapes=[
            pltpu.VMEM((heads, key_part + rotary, LANES), BF16),
            pltpu.VMEM((LANES * heads, size), BF16),
            pltpu.VMEM((LANES * heads, size), jnp.float32),
            dma((2,)),
        ],
        compiler_params=pltpu.CompilerParams(vmem_limit_bytes=16 * 1024 * 1024),
    )(*held)
    return keys[None], values.reshape(1, length, heads, size)


def solution(mesh):
    in_specs = (
        P("ens", ("ctx", "group"), None),
        P("ens", ("ctx", "group"), None),
        P(),
        P("ens", "group", None),
        P("ens", "group", None),
    )
    out_specs = (P(("ens", "ctx"), "group", None, None), P(("ens", "ctx"), None, "group", None))
    return jax.shard_map(
        per_device, mesh=mesh, in_specs=in_specs, out_specs=out_specs, check_vma=False
    )
```

```python
import functools

import jax
import jax.numpy as jnp
from jax import lax
from jax.experimental import pallas as pl
from jax.experimental.pallas import tpu as pltpu
from jax.sharding import PartitionSpec as P

MESH = pl.DeviceIdType.MESH
LANES = 128
BF16 = jnp.bfloat16
SHIFT, DELAY = False, False


def xor(me, step, count):
    total, bit = 0, 1
    while bit < count:
        total = total + bit * lax.rem(me // bit + step // bit, 2)
        bit *= 2
    return total


def partner(me, step, count):
    return lax.rem(me + step, count) if count & (count - 1) else xor(me, step, count)


def source(me, step, count):
    return lax.rem(me + count - step, count) if count & (count - 1) else xor(me, step, count)


def turn(i, count):
    return jnp.where(i == 1, count - 1, i - 1)


def pending(c, g, seqs, planes, units):
    q = source(c, turn(jnp.int32(seqs - 1), seqs), seqs) if seqs > 1 else c
    return q, jnp.where(2 * g < planes, units - 1, 0)


def expand(block, slabs, blk, per_unit, heads, rotary, gain, key_w, value_w, mixed, put_keys, put_values):
    key_part = key_w.shape[0] // heads
    size = value_w.shape[1] // heads
    x = jnp.concatenate(
        [block(k * blk, blk).astype(jnp.float32).reshape(LANES, LANES) for k in range(slabs)],
        axis=1,
    )
    mean = jnp.mean(x * x, axis=-1, keepdims=True)
    rows = (x * lax.rsqrt(mean + 1e-06) * gain[...]).astype(BF16)
    wide_keys = lax.dot_general(
        key_w[...], rows, (((1,), (1,)), ((), ())), preferred_element_type=jnp.float32
    ).astype(BF16)
    tails = block(slabs * blk, blk * rotary // LANES).astype(jnp.float32)
    pieces = []
    for j in range(per_unit):
        pieces += [tails[j][:, :rotary], pltpu.roll(tails[j], rotary, 1)[:, :rotary]]
    turned = jnp.concatenate(pieces, axis=0).T.astype(BF16)
    for h in range(heads):
        put_keys(h, wide_keys[h * key_part : (h + 1) * key_part], turned)
    wide_values = jnp.dot(rows, value_w[...], preferred_element_type=jnp.float32)
    for h in range(heads):
        mixed[pl.ds(h, LANES, stride=heads), :] = wide_values[:, h * size : (h + 1) * size]
    put_values(mixed[...].astype(BF16))


def kernel(
    seqs, planes, heads, rotary,
    lat, rot, gain_in, key_up, value_up,
    keys, values, last, key_w, value_w, gain,
    stage, raw, mid, rot_stage, key_stage, value_stage, wide, mixed,
    load_sem, got, mid_got, sent, ready,
):
    ens, c, g = lax.axis_index("ens"), lax.axis_index("ctx"), lax.axis_index("group")
    blk, latent = lat.shape[1:]
    slabs = latent // LANES
    tail = slabs * blk
    half = blk // 2
    per_unit = LANES // blk
    units = planes // per_unit
    key_part = key_w.shape[0] // heads
    size = value_w.shape[1] // heads
    first = partner(c, seqs - 1, seqs)

    def lat_load(s, k, sem):
        return pltpu.make_async_copy(
            lat.at[s, :, pl.ds(k * LANES, LANES)],
            stage.at[s, pl.ds(k * blk, blk), :],
            load_sem.at[sem],
        )

    rot_load = pltpu.make_async_copy(rot, rot_stage, load_sem.at[0])
    for k in range(slabs):
        lat_load(first, k, 1).start()
    rot_load.start()

    @pl.loop(1, seqs)
    def _(b):
        for k in range(slabs):
            lat_load(partner(first, b, seqs), k, 2).start()

    loads = [
        pltpu.make_async_copy(key_up, key_stage, load_sem.at[3]),
        pltpu.make_async_copy(value_up, value_stage, load_sem.at[4]),
        pltpu.make_async_copy(gain_in, gain, load_sem.at[4]),
    ]
    for load in loads:
        load.start()

    barrier = pltpu.get_barrier_semaphore()
    above, below = g < planes - 1, g > 0
    edge = (g == 0) | (g == planes - 1)

    def inner(way, far):
        return g > far if way == 0 else g + far < planes - 1

    @pl.when(above)
    def _():
        pl.semaphore_signal(barrier, inc=1, device_id={"group": g + 1}, device_id_type=MESH)

    @pl.loop(c + 1, seqs)
    def _(s):
        pl.semaphore_signal(barrier, inc=1, device_id={"ctx": s}, device_id_type=MESH)

    def remote(src, dst, in_sem, to):
        return pltpu.make_async_remote_copy(
            src_ref=src, dst_ref=dst, send_sem=sent, recv_sem=in_sem,
            device_id=to, device_id_type=MESH,
        )

    def out(way, i, s, part, to):
        return remote(
            stage.at[s, part], mid.at[way, 0, i - 1, part], mid_got.at[way, 0, i - 1], {"group": to}
        )

    def own_along(to):
        return remote(stage.at[c], raw.at[c, g], got.at[g, c], {"group": to})

    def own_side(s):
        return remote(stage.at[s], raw.at[c, g], got.at[g, c], {"ctx": s})

    def forward(way, i, to):
        return remote(mid.at[way, 0, i - 1], mid.at[way, 1, i - 1], mid_got.at[way, 1, i - 1], {"group": to})

    def scatter(way, far, i, p, s):
        return remote(mid.at[way, far, i - 1], raw.at[c, p], got.at[p, c], {"ctx": s})

    def relay(p, q, to):
        return remote(raw.at[q, p], raw.at[q, p], got.at[p, q], {"group": to})

    whole = pl.ds(0, stage.shape[1])
    wide_part, rot_part = pl.ds(0, tail), pl.ds(tail, half)

    def rest(way, to):
        @pl.loop(2, seqs)
        def _(i):
            out(way, i, partner(c, turn(i, seqs), seqs), whole, to).start()

    @pl.when(c + g > 0)
    def _():
        pl.semaphore_wait(barrier, c + jnp.minimum(g, 1))

    @pl.when(below)
    def _():
        pl.semaphore_signal(ready.at[0], inc=1, device_id={"group": g - 1}, device_id_type=MESH)

    @pl.loop(0, c)
    def _(s):
        pl.semaphore_signal(ready.at[1], inc=1, device_id={"ctx": s}, device_id_type=MESH)

    def prepare():
        loads[0].wait()
        wide[...] = key_stage[...].astype(jnp.float32)
        for h in range(heads):
            key_w[h * key_part : (h + 1) * key_part, :] = (
                wide[pl.ds(h, latent, stride=heads), :].T.astype(BF16)
            )
        loads[1].wait()
        loads[2].wait()
        wide[...] = value_stage[...].astype(jnp.float32)
        for h in range(heads):
            value_w[:, h * size : (h + 1) * size] = (
                wide[pl.ds(h, latent, stride=heads), :].astype(BF16)
            )

    if DELAY:
        pl.when(ens > 0)(prepare)

    for k in range(slabs):
        lat_load(first, k, 1).wait()

    @pl.when(below & above)
    def _():
        out(1, 1, first, wide_part, g - 1).start()

    rot_load.wait()

    @pl.loop(0, seqs)
    def _(s):
        block = rot_stage[s].astype(jnp.float32)
        both = jnp.concatenate([block[:half], block[half:]], axis=1)
        stage[s, pl.ds(tail, half), :] = both.astype(BF16)

    @pl.loop(1, seqs)
    def _(b):
        for k in range(slabs):
            lat_load(partner(first, b, seqs), k, 2).wait()

    @pl.when(below & above)
    def _():
        out(1, 1, first, rot_part, g - 1).start()
        rest(1, g - 1)
        pl.when(jnp.logical_not(inner(1, 1)))(lambda: own_along(g - 1).start())
        pl.semaphore_wait(ready.at[0], 1)
        out(0, 1, first, whole, g + 1).start()
        rest(0, g + 1)
        pl.when(jnp.logical_not(inner(0, 1)))(lambda: own_along(g + 1).start())

    @pl.when(below & (g == planes - 1))
    def _():
        own_along(g - 1).start()

    @pl.when(above & (g == 0))
    def _():
        pl.semaphore_wait(ready.at[0], 1)
        own_along(g + 1).start()

    @pl.when(c < seqs - 1)
    def _():
        pl.semaphore_wait(ready.at[1], seqs - 1 - c)

    @pl.loop(1, seqs)
    def _(i):
        own_side(partner(c, turn(i, seqs), seqs)).start()

    raw[c, g] = stage[c]
    pl.when(ens == 0)(prepare) if DELAY else prepare()

    low = 2 * g < planes

    def near_first(go):
        pl.when(low)(lambda: go(1))
        go(0)
        pl.when(jnp.logical_not(low))(lambda: go(1))

    def arrived(p, q):
        relay(p, q, g).wait_recv()

    def plane(way, far):
        return g - far if way == 0 else g + far

    def exists(way, far):
        return g >= far if way == 0 else g + far < planes

    def onward(way):
        return above if way == 0 else below

    def towards(way):
        return g + 1 if way == 0 else g - 1

    def along(far):
        def go(way):
            @pl.when(exists(way, far))
            def _():
                arrived(plane(way, far), c)

                @pl.when(onward(way))
                def _():
                    relay(plane(way, far), c, towards(way)).start()

        near_first(go)

    def direct(way, far, origin, i):
        if way == 0 or not SHIFT:
            return inner(way, far)
        return inner(way, far) & ((origin > 0) | (i > 1))

    def pass_mid(far, i):
        def go(way):
            @pl.when(inner(way, far) if far == 1 else direct(way, far, c, i))
            def _():
                forward(way, i, g).wait_recv() if far == 2 else out(way, i, c, whole, g).wait_recv()
                s = partner(c, turn(i, seqs), seqs)
                scatter(way, far - 1, i, plane(way, far), s).start()
                if far == 1:
                    @pl.when(onward(way) & direct(way, 1, c, i))
                    def _():
                        forward(way, i, towards(way)).start()

        near_first(go)

    def take(far, i):
        def go(way):
            @pl.when(exists(way, far))
            def _():
                q = source(c, turn(i, seqs), seqs)
                arrived(plane(way, far), q)

                @pl.when(onward(way) & ((far > 1) | jnp.logical_not(direct(way, 1, q, i))))
                def _():
                    relay(plane(way, far), q, towards(way)).start()

        near_first(go)

    end_q, end_u = pending(c, g, seqs, planes, units)

    def settle(q, low_far, high_far):
        @pl.loop(0, units)
        def _(u):
            far = jnp.maximum(g - u * per_unit, (u + 1) * per_unit - 1 - g)
            far = jnp.maximum(far, 1)
            wanted = (far >= low_far) & (far <= high_far)

            @pl.when(wanted & ((q != end_q) | (u != end_u)))
            def _():
                begin = u * per_unit
                start = pl.multiple_of((q * planes + begin) * blk, LANES)

                def block(row, count):
                    return raw[q, pl.ds(begin, per_unit), row : row + count, :]

                def put_keys(h, wide_keys, turned):
                    keys[h, :key_part, pl.ds(start, LANES)] = wide_keys
                    keys[h, key_part:, pl.ds(start, LANES)] = turned

                def put_values(rows):
                    at = pl.multiple_of(start * heads, LANES * heads)
                    values[pl.ds(at, LANES * heads), :] = rows

                expand(
                    block, slabs, blk, per_unit, heads, rotary, gain, key_w, value_w, mixed,
                    put_keys, put_values,
                )

    def own(i):
        q = source(c, turn(i, seqs), seqs)
        arrived(g, q)

        @pl.when(above & (g == 0))
        def _():
            relay(g, q, g + 1).start()

        @pl.when(below & (g == planes - 1))
        def _():
            relay(g, q, g - 1).start()

    @pl.loop(1, seqs)
    def _(i):
        pass_mid(1, i)
        pl.when(edge)(lambda: own(i))

    pl.when(inner(1, 1) & below)(lambda: own_along(g - 1).start())
    pl.when(inner(0, 1) & above)(lambda: own_along(g + 1).start())
    pl.when(jnp.logical_not(edge))(lambda: along(1))

    @pl.loop(1, seqs + 1)
    def _(i):
        @pl.when(i < seqs)
        def _():
            pass_mid(2, i)
            pl.when(jnp.logical_not(edge))(lambda: own(i))
            take(1, i)

        @pl.when(i == seqs)
        def _():
            pl.when(edge)(lambda: along(1))

        settle(jnp.where(i == seqs, c, source(c, turn(i, seqs), seqs)), 1, 1)

    along(2)

    @pl.loop(2, max(planes, 3))
    def _(far):
        @pl.loop(0, seqs)
        def _(i):
            @pl.when((i == 0) & (far > 2))
            def _():
                along(far)

            @pl.when(i > 0)
            def _():
                take(far, i)

            settle(jnp.where(i == 0, c, source(c, turn(i, seqs), seqs)), far, far)

    last[...] = raw[end_q, pl.ds(end_u * per_unit, per_unit)]

    ups, downs = jnp.minimum(planes - 1 - g, 1), jnp.minimum(g, 1)
    total = seqs * (ups + downs + g * ups + (planes - 1 - g) * downs)
    spread = sum(jnp.where(inner(way, far), 1, 0) for way in (0, 1) for far in (1, 2))
    total = total + (seqs - 1) * (1 + spread)
    if SHIFT:
        here, there = jnp.where(c == 0, 1, 0), jnp.where(c == seqs - 1, 1, 0)
        total = total + jnp.where(inner(1, 1) & below, there - here, 0) - jnp.where(inner(1, 2), here, 0)

    @pl.loop(0, total)
    def _(_):
        own_along(g).wait_send()


def store(
    seqs, planes, heads, rotary, blk,
    keys, values, last, key_w, value_w, gain,
    keys_out, values_out,
    end_keys, end_values, mixed, sems,
):
    c, g = lax.axis_index("ctx"), lax.axis_index("group")
    slabs = gain.shape[1] // LANES
    per_unit = LANES // blk
    units = planes // per_unit
    key_part = key_w.shape[0] // heads
    blocks = seqs * units
    end_q, end_u = pending(c, g, seqs, planes, units)
    end = end_q * units + end_u

    def columns(b):
        return pl.ds(pl.multiple_of(b * LANES, LANES), LANES)

    def rows(b):
        return pl.ds(pl.multiple_of(b * LANES * heads, LANES * heads), LANES * heads)

    @pl.loop(1, blocks)
    def _(j):
        b = lax.rem(end + j, blocks)
        pltpu.make_async_copy(
            keys.at[:, :, columns(b)], keys_out.at[:, :, columns(b)], sems.at[0]
        ).start()
        pltpu.make_async_copy(values.at[rows(b)], values_out.at[rows(b)], sems.at[1]).start()

    def block(row, count):
        return last[:, row : row + count, :]

    def put_keys(h, wide_keys, turned):
        end_keys[h, :key_part, :] = wide_keys
        end_keys[h, key_part:, :] = turned

    def put_values(part):
        end_values[...] = part

    expand(
        block, slabs, blk, per_unit, heads, rotary, gain, key_w, value_w, mixed,
        put_keys, put_values,
    )
    pltpu.make_async_copy(end_keys, keys_out.at[:, :, columns(end)], sems.at[0]).start()
    pltpu.make_async_copy(end_values, values_out.at[rows(end)], sems.at[1]).start()
    pltpu.make_async_copy(keys, keys_out, sems.at[0]).wait()
    pltpu.make_async_copy(values, values_out, sems.at[1]).wait()


def per_device(latents, rotary_rows, latent_gain, key_up, value_up):
    seqs, planes = lax.axis_size("ctx"), lax.axis_size("group")
    _, blk, latent = latents.shape
    rotary = rotary_rows.shape[2]
    heads, key_part = key_up.shape[1:]
    size = value_up.shape[2]
    length = seqs * planes * blk
    per_unit = LANES // blk
    packed = (blk * (latent + rotary) // LANES, LANES)
    dma = pltpu.SemaphoreType.DMA
    in_hbm = functools.partial(pltpu.with_memory_space_constraint, memory_space=pltpu.HBM)
    outer = pl.BlockSpec(memory_space=pltpu.HBM)
    inside = pl.BlockSpec(memory_space=pltpu.VMEM)
    held = pl.pallas_call(
        functools.partial(kernel, seqs, planes, heads, rotary),
        out_shape=(
            pltpu.VMEM((heads, key_part + rotary, length), BF16),
            pltpu.VMEM((length * heads, size), BF16),
            pltpu.VMEM((per_unit, *packed), BF16),
            pltpu.VMEM((heads * key_part, latent), BF16),
            pltpu.VMEM((latent, heads * size), BF16),
            pltpu.VMEM((1, latent), jnp.float32),
        ),
        in_specs=[outer] * 5,
        out_specs=(inside,) * 6,
        scratch_shapes=[
            pltpu.VMEM((seqs, *packed), BF16),
            pltpu.VMEM((seqs, planes, *packed), BF16),
            pltpu.VMEM((2, 2, seqs - 1, *packed), BF16),
            pltpu.VMEM((seqs, blk, rotary), BF16),
            pltpu.VMEM((latent * heads, key_part), BF16),
            pltpu.VMEM((latent * heads, size), BF16),
            pltpu.VMEM((latent * heads, size), jnp.float32),
            pltpu.VMEM((LANES * heads, size), jnp.float32),
            dma((5,)),
            dma((planes, seqs)),
            dma((2, 2, seqs - 1)),
            dma,
            pltpu.SemaphoreType.REGULAR((2,)),
        ],
        compiler_params=pltpu.CompilerParams(
            collective_id=0, has_side_effects=True, vmem_limit_bytes=32 * 1024 * 1024
        ),
    )(
        in_hbm(latents),
        in_hbm(rotary_rows),
        in_hbm(latent_gain.reshape(1, latent)),
        in_hbm(key_up.reshape(latent * heads, key_part)),
        in_hbm(value_up.reshape(latent * heads, size)),
    )
    keys, values = pl.pallas_call(
        functools.partial(store, seqs, planes, heads, rotary, blk),
        out_shape=(
            jax.ShapeDtypeStruct((heads, key_part + rotary, length), BF16),
            jax.ShapeDtypeStruct((length * heads, size), BF16),
        ),
        in_specs=[inside] * 6,
        out_specs=(outer, outer),
        scratch_shapes=[
            pltpu.VMEM((heads, key_part + rotary, LANES), BF16),
            pltpu.VMEM((LANES * heads, size), BF16),
            pltpu.VMEM((LANES * heads, size), jnp.float32),
            dma((2,)),
        ],
        compiler_params=pltpu.CompilerParams(vmem_limit_bytes=16 * 1024 * 1024),
    )(*held)
    return keys[None], values.reshape(1, length, heads, size)


def solution(mesh):
    in_specs = (
        P("ens", ("ctx", "group"), None),
        P("ens", ("ctx", "group"), None),
        P(),
        P("ens", "group", None),
        P("ens", "group", None),
    )
    out_specs = (P(("ens", "ctx"), "group", None, None), P(("ens", "ctx"), None, "group", None))
    return jax.shard_map(
        per_device, mesh=mesh, in_specs=in_specs, out_specs=out_specs, check_vma=False
    )
```

```python
import functools

import jax
import jax.numpy as jnp
from jax import lax
from jax.experimental import pallas as pl
from jax.experimental.pallas import tpu as pltpu
from jax.sharding import PartitionSpec as P

MESH = pl.DeviceIdType.MESH
LANES = 128
BF16 = jnp.bfloat16
SHIFT = 1
HELD = 0


def xor(me, step, count):
    total, bit = 0, 1
    while bit < count:
        total = total + bit * lax.rem(me // bit + step // bit, 2)
        bit *= 2
    return total


def partner(me, step, count):
    return lax.rem(me + step, count) if count & (count - 1) else xor(me, step, count)


def source(me, step, count):
    return lax.rem(me + count - step, count) if count & (count - 1) else xor(me, step, count)


def join(a, b, count):
    if count & (count - 1):
        return jnp.maximum(a, b)
    total, bit = 0, 1
    while bit < count:
        total = total + bit * jnp.maximum(lax.rem(a // bit, 2), lax.rem(b // bit, 2))
        bit *= 2
    return total


def lower(c, count):
    if count & (count - 1):
        return c
    total, bit = 1, 1
    while bit < count:
        total = total * (1 + lax.rem(c // bit, 2))
        bit *= 2
    return total - 1


def pending(c, g, seqs, planes, units):
    q = source(c, seqs - 1, seqs) if seqs > 1 else c
    return q, jnp.where(2 * g < planes, units - 1, 0)


def expand(block, slabs, blk, per_unit, heads, rotary, gain, key_w, value_w, mixed, put_keys, put_values):
    key_part = key_w.shape[0] // heads
    size = value_w.shape[1] // heads
    x = jnp.concatenate(
        [block(k * blk, blk).astype(jnp.float32).reshape(LANES, LANES) for k in range(slabs)],
        axis=1,
    )
    mean = jnp.mean(x * x, axis=-1, keepdims=True)
    rows = (x * lax.rsqrt(mean + 1e-06) * gain[...]).astype(BF16)
    wide_keys = lax.dot_general(
        key_w[...], rows, (((1,), (1,)), ((), ())), preferred_element_type=jnp.float32
    ).astype(BF16)
    tails = block(slabs * blk, blk * rotary // LANES).astype(jnp.float32)
    pieces = []
    for j in range(per_unit):
        pieces += [tails[j][:, :rotary], pltpu.roll(tails[j], rotary, 1)[:, :rotary]]
    turned = jnp.concatenate(pieces, axis=0).T.astype(BF16)
    for h in range(heads):
        put_keys(h, wide_keys[h * key_part : (h + 1) * key_part], turned)
    wide_values = jnp.dot(rows, value_w[...], preferred_element_type=jnp.float32)
    for h in range(heads):
        mixed[pl.ds(h, LANES, stride=heads), :] = wide_values[:, h * size : (h + 1) * size]
    put_values(mixed[...].astype(BF16))


def kernel(
    seqs, planes, heads, rotary,
    lat, rot, gain_in, key_up, value_up,
    keys, values, last, key_w, value_w, gain,
    stage, raw, mid, rot_stage, key_stage, value_stage, wide, mixed,
    load_sem, got, mid_got, sent, ready,
):
    ens, c, g = lax.axis_index("ens"), lax.axis_index("ctx"), lax.axis_index("group")
    blk, latent = lat.shape[1:]
    slabs = latent // LANES
    tail = slabs * blk
    half = blk // 2
    ways = mid.shape[0]
    per_unit = LANES // blk
    units = planes // per_unit
    key_part = key_w.shape[0] // heads
    size = value_w.shape[1] // heads
    first = partner(c, 1, seqs)

    def lat_load(s, k, sem):
        return pltpu.make_async_copy(
            lat.at[s, :, pl.ds(k * LANES, LANES)],
            stage.at[s, pl.ds(k * blk, blk), :],
            load_sem.at[sem],
        )

    rot_load = pltpu.make_async_copy(rot, rot_stage, load_sem.at[0])
    for k in range(slabs):
        lat_load(first, k, 1).start()
    rot_load.start()

    @pl.loop(1, seqs)
    def _(b):
        for k in range(slabs):
            lat_load(partner(first, b, seqs), k, 2).start()

    loads = [
        pltpu.make_async_copy(key_up, key_stage, load_sem.at[3]),
        pltpu.make_async_copy(value_up, value_stage, load_sem.at[3]),
        pltpu.make_async_copy(gain_in, gain, load_sem.at[3]),
    ]
    for load in loads:
        load.start()

    barrier = pltpu.get_barrier_semaphore()
    above, below = g < planes - 1, g > 0
    edge = (g == 0) | (g == planes - 1)
    gate = (g == 1) | (g == planes - 2) if planes > 3 and HELD else g < 0

    def inner(way, far):
        return g > far if way == 0 else g + far < planes - 1

    @pl.when(above)
    def _():
        pl.semaphore_signal(barrier, inc=1, device_id={"group": g + 1}, device_id_type=MESH)

    @pl.when(gate & (ens == 1))
    def _():
        pl.semaphore_signal(barrier, inc=1, device_id={"ens": 0}, device_id_type=MESH)

    @pl.loop(c + 1, seqs)
    def _(s):
        @pl.when(join(c, s, seqs) == s)
        def _():
            pl.semaphore_signal(barrier, inc=1, device_id={"ctx": s}, device_id_type=MESH)

    def remote(src, dst, in_sem, to):
        return pltpu.make_async_remote_copy(
            src_ref=src, dst_ref=dst, send_sem=sent, recv_sem=in_sem,
            device_id=to, device_id_type=MESH,
        )

    def out(way, i, s, part, to):
        return remote(
            stage.at[s, part], mid.at[way % ways, 0, i - 1, part], mid_got.at[way % ways, 0, i - 1], {"group": to}
        )

    def own_along(to):
        return remote(stage.at[c], raw.at[c, g], got.at[g, c], {"group": to})

    def own_side(s):
        return remote(stage.at[s], raw.at[c, g], got.at[g, c], {"ctx": s})

    def forward(way, i, to):
        return remote(mid.at[way % ways, 0, i - 1], mid.at[way % ways, 1, i - 1], mid_got.at[way % ways, 1, i - 1], {"group": to})

    def scatter(way, far, i, p, s):
        return remote(mid.at[way % ways, far, i - 1], raw.at[c, p], got.at[p, c], {"ctx": s})

    def relay(p, q, to):
        return remote(raw.at[q, p], raw.at[q, p], got.at[p, q], {"group": to})

    whole = pl.ds(0, stage.shape[1])
    wide_part, rot_part = pl.ds(0, tail), pl.ds(tail, half)

    def rest(way, to):
        @pl.loop(2, seqs)
        def _(i):
            out(way, i, partner(c, i, seqs), whole, to).start()

    early = lower(c, seqs) + jnp.minimum(g, 1) + jnp.where(gate & (ens == 0), 1, 0)

    @pl.when(early > 0)
    def _():
        pl.semaphore_wait(barrier, early)

    @pl.when(below)
    def _():
        pl.semaphore_signal(ready.at[0], inc=1, device_id={"group": g - 1}, device_id_type=MESH)

    @pl.loop(0, c)
    def _(s):
        @pl.when(join(c, s, seqs) == c)
        def _():
            pl.semaphore_signal(ready.at[2 + c], inc=1, device_id={"ctx": s}, device_id_type=MESH)

    def prepare():
        for load in loads:
            load.wait()
        wide[...] = key_stage[...].astype(jnp.float32)
        for h in range(heads):
            key_w[h * key_part : (h + 1) * key_part, :] = (
                wide[pl.ds(h, latent, stride=heads), :].T.astype(BF16)
            )
        wide[...] = value_stage[...].astype(jnp.float32)
        for h in range(heads):
            value_w[:, h * size : (h + 1) * size] = (
                wide[pl.ds(h, latent, stride=heads), :].astype(BF16)
            )

    for k in range(slabs):
        lat_load(first, k, 1).wait()

    @pl.when(below & above)
    def _():
        out(1, 1, first, wide_part, g - 1).start()

    rot_load.wait()

    @pl.loop(0, seqs)
    def _(s):
        block = rot_stage[s].astype(jnp.float32)
        both = jnp.concatenate([block[:half], block[half:]], axis=1)
        stage[s, pl.ds(tail, half), :] = both.astype(BF16)

    @pl.loop(1, seqs)
    def _(b):
        for k in range(slabs):
            lat_load(partner(first, b, seqs), k, 2).wait()

    @pl.when(below & above)
    def _():
        out(1, 1, first, rot_part, g - 1).start()
        rest(1, g - 1)
        pl.when(jnp.logical_not(inner(1, 1)))(lambda: own_along(g - 1).start())
        pl.semaphore_wait(ready.at[0], 1)
        out(0, 1, first, whole, g + 1).start()
        rest(0, g + 1)
        pl.when(jnp.logical_not(inner(0, 1)))(lambda: own_along(g + 1).start())

    @pl.when(below & (g == planes - 1))
    def _():
        own_along(g - 1).start()

    @pl.when(above & (g == 0))
    def _():
        pl.semaphore_wait(ready.at[0], 1)
        own_along(g + 1).start()

    @pl.loop(c, seqs)
    def _(t):
        @pl.when(join(c, t, seqs) == t)
        def _():
            @pl.when(t > c)
            def _():
                pl.semaphore_wait(ready.at[2 + t], 1)

            @pl.loop(1, seqs)
            def _(i):
                s = partner(c, i, seqs)

                @pl.when(join(c, s, seqs) == t)
                def _():
                    own_side(s).start()

    raw[c, g] = stage[c]
    prepare()

    low = 2 * g < planes

    def near_first(go):
        pl.when(low)(lambda: go(1))
        go(0)
        pl.when(jnp.logical_not(low))(lambda: go(1))

    def arrived(p, q):
        relay(p, q, g).wait_recv()

    def plane(way, far):
        return g - far if way == 0 else g + far

    def exists(way, far):
        return g >= far if way == 0 else g + far < planes

    def onward(way):
        return above if way == 0 else below

    def towards(way):
        return g + 1 if way == 0 else g - 1

    def along(far):
        def go(way):
            @pl.when(exists(way, far))
            def _():
                arrived(plane(way, far), c)

                @pl.when(onward(way))
                def _():
                    relay(plane(way, far), c, towards(way)).start()

        near_first(go)

    def direct(way, far, origin, i):
        if way == 0 or not SHIFT:
            return inner(way, far)
        return inner(way, far) & ((origin > 0) | (i != SHIFT) | (ens > 0))

    def pass_mid(far, i):
        def go(way):
            @pl.when(inner(way, far) if far == 1 else direct(way, far, c, i))
            def _():
                forward(way, i, g).wait_recv() if far == 2 else out(way, i, c, whole, g).wait_recv()
                s = partner(c, i, seqs)
                scatter(way, far - 1, i, plane(way, far), s).start()
                if far == 1:
                    @pl.when(onward(way) & direct(way, 1, c, i))
                    def _():
                        forward(way, i, towards(way)).start()

        near_first(go)

    def take(far, i, chain=None):
        def go(way):
            wanted = exists(way, far)
            if chain is not None:
                wanted = wanted & (inner(way, far) != chain)

            @pl.when(wanted)
            def _():
                q = source(c, i, seqs)
                arrived(plane(way, far), q)

                @pl.when(onward(way) & ((far > 1) | jnp.logical_not(direct(way, 1, q, i))))
                def _():
                    relay(plane(way, far), q, towards(way)).start()

        near_first(go)

    end_q, end_u = pending(c, g, seqs, planes, units)

    def settle(q, low_far, high_far):
        @pl.loop(0, units)
        def _(u):
            far = jnp.maximum(g - u * per_unit, (u + 1) * per_unit - 1 - g)
            far = jnp.maximum(far, 1)
            wanted = (far >= low_far) & (far <= high_far)

            @pl.when(wanted & ((q != end_q) | (u != end_u)))
            def _():
                begin = u * per_unit
                start = pl.multiple_of((q * planes + begin) * blk, LANES)

                def block(row, count):
                    return raw[q, pl.ds(begin, per_unit), row : row + count, :]

                def put_keys(h, wide_keys, turned):
                    keys[h, :key_part, pl.ds(start, LANES)] = wide_keys
                    keys[h, key_part:, pl.ds(start, LANES)] = turned

                def put_values(rows):
                    at = pl.multiple_of(start * heads, LANES * heads)
                    values[pl.ds(at, LANES * heads), :] = rows

                expand(
                    block, slabs, blk, per_unit, heads, rotary, gain, key_w, value_w, mixed,
                    put_keys, put_values,
                )

    def own(i):
        q = source(c, i, seqs)
        arrived(g, q)

        @pl.when(above & (g == 0))
        def _():
            relay(g, q, g + 1).start()

        @pl.when(below & (g == planes - 1))
        def _():
            relay(g, q, g - 1).start()

    @pl.loop(1, seqs)
    def _(i):
        pl.when(g == planes - 1)(lambda: own(i))
        pl.when((g < planes - 1) | (g == 0))(lambda: pass_mid(1, i))
        pl.when((g == 0) & above)(lambda: own(i))

    @pl.loop(1, seqs)
    def _(i):
        pl.when((g == planes - 1) & below)(lambda: pass_mid(1, i))

    pl.when(inner(1, 1) & below)(lambda: own_along(g - 1).start())
    pl.when(inner(0, 1) & above)(lambda: own_along(g + 1).start())
    pl.when(jnp.logical_not(edge))(lambda: along(1))

    @pl.when(jnp.logical_not(edge))
    def _():
        settle(c, 1, 1)

        @pl.loop(1, seqs)
        def _(i):
            take(1, i, True)

    @pl.loop(1, seqs + 1)
    def _(i):
        @pl.when(i < seqs)
        def _():
            pass_mid(2, i)
            pl.when(jnp.logical_not(edge))(lambda: own(i))
            pl.when(edge)(lambda: take(1, i))
            pl.when(jnp.logical_not(edge))(lambda: take(1, i, False))

        @pl.when((i == seqs) & edge)
        def _():
            along(1)

        @pl.when((i < seqs) | edge)
        def _():
            settle(jnp.where(i == seqs, c, source(c, i, seqs)), 1, 1)

    along(2)

    @pl.loop(2, max(planes, 3))
    def _(far):
        @pl.loop(0, seqs)
        def _(i):
            @pl.when((i == 0) & (far > 2))
            def _():
                along(far)

            turn = gate & (far == planes - 2)

            @pl.when(turn & (ens == 1) & (i == max(seqs - HELD, 1)))
            def _():
                pl.semaphore_wait(ready.at[1], 1)

            @pl.when(i > 0)
            def _():
                take(far, i)

            @pl.when(turn & (ens == 0) & (i == seqs - 1))
            def _():
                pl.semaphore_signal(ready.at[1], inc=1, device_id={"ens": 1}, device_id_type=MESH)

            settle(jnp.where(i == 0, c, source(c, i, seqs)), far, far)

    last[...] = raw[end_q, pl.ds(end_u * per_unit, per_unit)]

    ups, downs = jnp.minimum(planes - 1 - g, 1), jnp.minimum(g, 1)
    total = seqs * (ups + downs + g * ups + (planes - 1 - g) * downs)
    spread = sum(jnp.where(inner(way, far), 1, 0) for way in (0, 1) for far in (1, 2))
    total = total + (seqs - 1) * (1 + spread)
    if SHIFT:
        here, there = jnp.where(c == 0, 1, 0), jnp.where(c == partner(0, SHIFT, seqs), 1, 0)
        change = jnp.where(inner(1, 1) & below, there - here, 0) - jnp.where(inner(1, 2), here, 0)
        total = total + jnp.where(ens == 0, change, 0)

    @pl.loop(0, total)
    def _(_):
        own_along(g).wait_send()


def store(
    seqs, planes, heads, rotary, blk,
    keys, values, last, key_w, value_w, gain,
    keys_out, values_out,
    end_keys, end_values, mixed, sems,
):
    c, g = lax.axis_index("ctx"), lax.axis_index("group")
    slabs = gain.shape[1] // LANES
    per_unit = LANES // blk
    units = planes // per_unit
    key_part = key_w.shape[0] // heads
    blocks = seqs * units
    end_q, end_u = pending(c, g, seqs, planes, units)
    end = end_q * units + end_u

    def columns(b):
        return pl.ds(pl.multiple_of(b * LANES, LANES), LANES)

    def rows(b):
        return pl.ds(pl.multiple_of(b * LANES * heads, LANES * heads), LANES * heads)

    @pl.loop(1, blocks)
    def _(j):
        b = lax.rem(end + j, blocks)
        pltpu.make_async_copy(
            keys.at[:, :, columns(b)], keys_out.at[:, :, columns(b)], sems.at[0]
        ).start()
        pltpu.make_async_copy(values.at[rows(b)], values_out.at[rows(b)], sems.at[1]).start()

    def block(row, count):
        return last[:, row : row + count, :]

    def put_keys(h, wide_keys, turned):
        end_keys[h, :key_part, :] = wide_keys
        end_keys[h, key_part:, :] = turned

    def put_values(part):
        end_values[...] = part

    expand(
        block, slabs, blk, per_unit, heads, rotary, gain, key_w, value_w, mixed,
        put_keys, put_values,
    )
    pltpu.make_async_copy(end_keys, keys_out.at[:, :, columns(end)], sems.at[0]).start()
    pltpu.make_async_copy(end_values, values_out.at[rows(end)], sems.at[1]).start()
    pltpu.make_async_copy(keys, keys_out, sems.at[0]).wait()
    pltpu.make_async_copy(values, values_out, sems.at[1]).wait()


def per_device(latents, rotary_rows, latent_gain, key_up, value_up):
    seqs, planes = lax.axis_size("ctx"), lax.axis_size("group")
    _, blk, latent = latents.shape
    rotary = rotary_rows.shape[2]
    heads, key_part = key_up.shape[1:]
    size = value_up.shape[2]
    length = seqs * planes * blk
    per_unit = LANES // blk
    ways = 1 if planes <= 4 else 2
    packed = (blk * (latent + rotary) // LANES, LANES)
    dma = pltpu.SemaphoreType.DMA
    in_hbm = functools.partial(pltpu.with_memory_space_constraint, memory_space=pltpu.HBM)
    outer = pl.BlockSpec(memory_space=pltpu.HBM)
    inside = pl.BlockSpec(memory_space=pltpu.VMEM)
    held = pl.pallas_call(
        functools.partial(kernel, seqs, planes, heads, rotary),
        out_shape=(
            pltpu.VMEM((heads, key_part + rotary, length), BF16),
            pltpu.VMEM((length * heads, size), BF16),
            pltpu.VMEM((per_unit, *packed), BF16),
            pltpu.VMEM((heads * key_part, latent), BF16),
            pltpu.VMEM((latent, heads * size), BF16),
            pltpu.VMEM((1, latent), jnp.float32),
        ),
        in_specs=[outer] * 5,
        out_specs=(inside,) * 6,
        scratch_shapes=[
            pltpu.VMEM((seqs, *packed), BF16),
            pltpu.VMEM((seqs, planes, *packed), BF16),
            pltpu.VMEM((ways, 2, seqs - 1, *packed), BF16),
            pltpu.VMEM((seqs, blk, rotary), BF16),
            pltpu.VMEM((latent * heads, key_part), BF16),
            pltpu.VMEM((latent * heads, size), BF16),
            pltpu.VMEM((latent * heads, size), jnp.float32),
            pltpu.VMEM((LANES * heads, size), jnp.float32),
            dma((4,)),
            dma((planes, seqs)),
            dma((ways, 2, seqs - 1)),
            dma,
            pltpu.SemaphoreType.REGULAR((2 + seqs,)),
        ],
        compiler_params=pltpu.CompilerParams(
            collective_id=0, has_side_effects=True, vmem_limit_bytes=32 * 1024 * 1024
        ),
    )(
        in_hbm(latents),
        in_hbm(rotary_rows),
        in_hbm(latent_gain.reshape(1, latent)),
        in_hbm(key_up.reshape(latent * heads, key_part)),
        in_hbm(value_up.reshape(latent * heads, size)),
    )
    keys, values = pl.pallas_call(
        functools.partial(store, seqs, planes, heads, rotary, blk),
        out_shape=(
            jax.ShapeDtypeStruct((heads, key_part + rotary, length), BF16),
            jax.ShapeDtypeStruct((length * heads, size), BF16),
        ),
        in_specs=[inside] * 6,
        out_specs=(outer, outer),
        scratch_shapes=[
            pltpu.VMEM((heads, key_part + rotary, LANES), BF16),
            pltpu.VMEM((LANES * heads, size), BF16),
            pltpu.VMEM((LANES * heads, size), jnp.float32),
            dma((2,)),
        ],
        compiler_params=pltpu.CompilerParams(vmem_limit_bytes=16 * 1024 * 1024),
    )(*held)
    return keys[None], values.reshape(1, length, heads, size)


def solution(mesh):
    in_specs = (
        P("ens", ("ctx", "group"), None),
        P("ens", ("ctx", "group"), None),
        P(),
        P("ens", "group", None),
        P("ens", "group", None),
    )
    out_specs = (P(("ens", "ctx"), "group", None, None), P(("ens", "ctx"), None, "group", None))
    return jax.shard_map(
        per_device, mesh=mesh, in_specs=in_specs, out_specs=out_specs, check_vma=False
    )
```

```python
import functools

import jax
import jax.numpy as jnp
from jax import lax
from jax.experimental import pallas as pl
from jax.experimental.pallas import tpu as pltpu
from jax.sharding import PartitionSpec as P

MESH = pl.DeviceIdType.MESH
LANES = 128
BF16 = jnp.bfloat16
GIVEN = 4, 18
HELD = 1


def xor(me, step, count):
    total, bit = 0, 1
    while bit < count:
        total = total + bit * lax.rem(me // bit + step // bit, 2)
        bit *= 2
    return total


def partner(me, step, count):
    return lax.rem(me + step, count) if count & (count - 1) else xor(me, step, count)


def source(me, step, count):
    return lax.rem(me + count - step, count) if count & (count - 1) else xor(me, step, count)


def join(a, b, count):
    if count & (count - 1):
        return jnp.maximum(a, b)
    total, bit = 0, 1
    while bit < count:
        total = total + bit * jnp.maximum(lax.rem(a // bit, 2), lax.rem(b // bit, 2))
        bit *= 2
    return total


def lower(c, count):
    if count & (count - 1):
        return c
    total, bit = 1, 1
    while bit < count:
        total = total * (1 + lax.rem(c // bit, 2))
        bit *= 2
    return total - 1


def pending(c, g, seqs, planes, units):
    q = source(c, seqs - 1, seqs) if seqs > 1 else c
    return q, jnp.where(2 * g < planes, units - 1, 0)


def expand(block, slabs, blk, per_unit, heads, rotary, gain, key_w, value_w, mixed, put_keys, put_values):
    key_part = key_w.shape[0] // heads
    size = value_w.shape[1] // heads
    x = jnp.concatenate(
        [block(k * blk, blk).astype(jnp.float32).reshape(LANES, LANES) for k in range(slabs)],
        axis=1,
    )
    mean = jnp.mean(x * x, axis=-1, keepdims=True)
    rows = (x * lax.rsqrt(mean + 1e-06) * gain[...]).astype(BF16)
    wide_keys = lax.dot_general(
        key_w[...], rows, (((1,), (1,)), ((), ())), preferred_element_type=jnp.float32
    ).astype(BF16)
    tails = block(slabs * blk, blk * rotary // LANES).astype(jnp.float32)
    pieces = []
    for j in range(per_unit):
        pieces += [tails[j][:, :rotary], pltpu.roll(tails[j], rotary, 1)[:, :rotary]]
    turned = jnp.concatenate(pieces, axis=0).T.astype(BF16)
    for h in range(heads):
        put_keys(h, wide_keys[h * key_part : (h + 1) * key_part], turned)
    wide_values = jnp.dot(rows, value_w[...], preferred_element_type=jnp.float32)
    for h in range(heads):
        mixed[pl.ds(h, LANES, stride=heads), :] = wide_values[:, h * size : (h + 1) * size]
    put_values(mixed[...].astype(BF16))


def kernel(
    seqs, planes, heads, rotary,
    lat, rot, gain_in, key_up, value_up,
    keys, values, last, key_w, value_w, gain,
    stage, raw, mid, rot_stage, key_stage, value_stage, wide, mixed,
    load_sem, got, mid_got, sent, ready,
):
    ens, c, g = lax.axis_index("ens"), lax.axis_index("ctx"), lax.axis_index("group")
    blk, latent = lat.shape[1:]
    slabs = latent // LANES
    tail = slabs * blk
    half = blk // 2
    give = stage.shape[1] // 16 * GIVEN[0] // GIVEN[1] * 16
    keep = stage.shape[1] - give
    kept, given = pl.ds(0, keep), pl.ds(keep, give)
    ways = mid.shape[0]
    per_unit = LANES // blk
    units = planes // per_unit
    key_part = key_w.shape[0] // heads
    size = value_w.shape[1] // heads
    first = partner(c, 1, seqs)

    def lat_load(s, k, sem):
        return pltpu.make_async_copy(
            lat.at[s, :, pl.ds(k * LANES, LANES)],
            stage.at[s, pl.ds(k * blk, blk), :],
            load_sem.at[sem],
        )

    rot_load = pltpu.make_async_copy(rot, rot_stage, load_sem.at[0])
    for k in range(slabs):
        lat_load(first, k, 1).start()
    rot_load.start()

    @pl.loop(1, seqs)
    def _(b):
        for k in range(slabs):
            lat_load(partner(first, b, seqs), k, 2).start()

    loads = [
        pltpu.make_async_copy(key_up, key_stage, load_sem.at[3]),
        pltpu.make_async_copy(value_up, value_stage, load_sem.at[3]),
        pltpu.make_async_copy(gain_in, gain, load_sem.at[3]),
    ]
    for load in loads:
        load.start()

    barrier = pltpu.get_barrier_semaphore()
    above, below = g < planes - 1, g > 0
    edge = (g == 0) | (g == planes - 1)
    gate = (g == 1) | (g == planes - 2) if planes > 3 and HELD else g < 0

    def inner(way, far):
        return g > far if way == 0 else g + far < planes - 1

    @pl.when(above)
    def _():
        pl.semaphore_signal(barrier, inc=1, device_id={"group": g + 1}, device_id_type=MESH)

    @pl.when(gate & (ens == 1))
    def _():
        pl.semaphore_signal(barrier, inc=1, device_id={"ens": 0}, device_id_type=MESH)

    @pl.loop(c + 1, seqs)
    def _(s):
        @pl.when(join(c, s, seqs) == s)
        def _():
            pl.semaphore_signal(barrier, inc=1, device_id={"ctx": s}, device_id_type=MESH)

    def remote(src, dst, in_sem, to):
        return pltpu.make_async_remote_copy(
            src_ref=src, dst_ref=dst, send_sem=sent, recv_sem=in_sem,
            device_id=to, device_id_type=MESH,
        )

    def out(way, i, s, part, to):
        return remote(
            stage.at[s, part], mid.at[way % ways, 0, i - 1, part], mid_got.at[way % ways, 0, i - 1], {"group": to}
        )

    def own_along(to):
        return remote(stage.at[c], raw.at[c, g], got.at[g, c], {"group": to})

    def own_side(s):
        return remote(stage.at[s], raw.at[c, g], got.at[g, c], {"ctx": s})

    def forward(way, i, part, to):
        return remote(
            mid.at[way % ways, 0, i - 1, part], mid.at[way % ways, 1, i - 1, part],
            mid_got.at[way % ways, 1, i - 1], {"group": to},
        )

    def scatter(way, far, i, part, p, s):
        return remote(mid.at[way % ways, far, i - 1, part], raw.at[c, p, part], got.at[p, c], {"ctx": s})

    def relay(p, q, to):
        return remote(raw.at[q, p], raw.at[q, p], got.at[p, q], {"group": to})

    def relay_given(p, q, to):
        return remote(raw.at[q, p, given], raw.at[q, p, given], got.at[p, q], {"group": to})

    whole = pl.ds(0, stage.shape[1])
    wide_part, rot_part = pl.ds(0, tail), pl.ds(tail, half)

    def rest(way, to):
        @pl.loop(2, seqs)
        def _(i):
            out(way, i, partner(c, i, seqs), whole, to).start()

    early = lower(c, seqs) + jnp.minimum(g, 1) + jnp.where(gate & (ens == 0), 1, 0)

    @pl.when(early > 0)
    def _():
        pl.semaphore_wait(barrier, early)

    @pl.when(below)
    def _():
        pl.semaphore_signal(ready.at[0], inc=1, device_id={"group": g - 1}, device_id_type=MESH)

    @pl.loop(0, c)
    def _(s):
        @pl.when(join(c, s, seqs) == c)
        def _():
            pl.semaphore_signal(ready.at[2 + c], inc=1, device_id={"ctx": s}, device_id_type=MESH)

    def prepare():
        for load in loads:
            load.wait()
        wide[...] = key_stage[...].astype(jnp.float32)
        for h in range(heads):
            key_w[h * key_part : (h + 1) * key_part, :] = (
                wide[pl.ds(h, latent, stride=heads), :].T.astype(BF16)
            )
        wide[...] = value_stage[...].astype(jnp.float32)
        for h in range(heads):
            value_w[:, h * size : (h + 1) * size] = (
                wide[pl.ds(h, latent, stride=heads), :].astype(BF16)
            )

    for k in range(slabs):
        lat_load(first, k, 1).wait()

    @pl.when(below & above)
    def _():
        out(1, 1, first, wide_part, g - 1).start()

    rot_load.wait()

    @pl.loop(0, seqs)
    def _(s):
        block = rot_stage[s].astype(jnp.float32)
        both = jnp.concatenate([block[:half], block[half:]], axis=1)
        stage[s, pl.ds(tail, half), :] = both.astype(BF16)

    @pl.loop(1, seqs)
    def _(b):
        for k in range(slabs):
            lat_load(partner(first, b, seqs), k, 2).wait()

    @pl.when(below & above)
    def _():
        out(1, 1, first, rot_part, g - 1).start()
        rest(1, g - 1)
        pl.when(jnp.logical_not(inner(1, 1)))(lambda: own_along(g - 1).start())
        pl.semaphore_wait(ready.at[0], 1)
        out(0, 1, first, whole, g + 1).start()
        rest(0, g + 1)
        pl.when(jnp.logical_not(inner(0, 1)))(lambda: own_along(g + 1).start())

    @pl.when(below & (g == planes - 1))
    def _():
        own_along(g - 1).start()

    @pl.when(above & (g == 0))
    def _():
        pl.semaphore_wait(ready.at[0], 1)
        own_along(g + 1).start()

    @pl.loop(c, seqs)
    def _(t):
        @pl.when(join(c, t, seqs) == t)
        def _():
            @pl.when(t > c)
            def _():
                pl.semaphore_wait(ready.at[2 + t], 1)

            @pl.loop(1, seqs)
            def _(i):
                s = partner(c, i, seqs)

                @pl.when(join(c, s, seqs) == t)
                def _():
                    own_side(s).start()

    raw[c, g] = stage[c]
    prepare()

    low = 2 * g < planes

    def near_first(go):
        pl.when(low)(lambda: go(1))
        go(0)
        pl.when(jnp.logical_not(low))(lambda: go(1))

    def arrived(p, q):
        relay(p, q, g).wait_recv()

    def plane(way, far):
        return g - far if way == 0 else g + far

    def exists(way, far):
        return g >= far if way == 0 else g + far < planes

    def onward(way):
        return above if way == 0 else below

    def towards(way):
        return g + 1 if way == 0 else g - 1

    def along(far):
        def go(way):
            @pl.when(exists(way, far))
            def _():
                arrived(plane(way, far), c)

                @pl.when(onward(way))
                def _():
                    relay(plane(way, far), c, towards(way)).start()

        near_first(go)

    def sized(way, go):
        if way == 0 or not give:
            go(whole)
        else:
            pl.when(c > 0)(lambda: go(whole))
            pl.when(c == 0)(lambda: go(kept))

    def pass_mid(far, i):
        def go(way):
            s = partner(c, i, seqs)

            @pl.when(inner(way, far))
            def _():
                if far == 1:
                    out(way, i, c, whole, g).wait_recv()
                    scatter(way, 0, i, whole, plane(way, far), s).start()

                    @pl.when(onward(way))
                    def _():
                        sized(way, lambda part: forward(way, i, part, towards(way)).start())
                else:
                    def onto(part):
                        forward(way, i, part, g).wait_recv()
                        scatter(way, 1, i, part, plane(way, far), s).start()

                    sized(way, onto)

        near_first(go)

    def take(far, i, chain=None):
        def go(way):
            wanted = exists(way, far)
            if chain is not None:
                wanted = wanted & (inner(way, far) != chain)

            @pl.when(wanted)
            def _():
                q = source(c, i, seqs)
                arrived(plane(way, far), q)

                @pl.when(onward(way) & ((far > 1) | jnp.logical_not(inner(way, 1))))
                def _():
                    relay(plane(way, far), q, towards(way)).start()

                if way == 1 and give:
                    @pl.when(below & inner(1, 1) & (far == 1) & (q == 0))
                    def _():
                        relay_given(plane(way, far), q, g - 1).start()

        near_first(go)

    end_q, end_u = pending(c, g, seqs, planes, units)

    def settle(q, low_far, high_far):
        @pl.loop(0, units)
        def _(u):
            far = jnp.maximum(g - u * per_unit, (u + 1) * per_unit - 1 - g)
            far = jnp.maximum(far, 1)
            wanted = (far >= low_far) & (far <= high_far)

            @pl.when(wanted & ((q != end_q) | (u != end_u)))
            def _():
                begin = u * per_unit
                start = pl.multiple_of((q * planes + begin) * blk, LANES)

                def block(row, count):
                    return raw[q, pl.ds(begin, per_unit), row : row + count, :]

                def put_keys(h, wide_keys, turned):
                    keys[h, :key_part, pl.ds(start, LANES)] = wide_keys
                    keys[h, key_part:, pl.ds(start, LANES)] = turned

                def put_values(rows):
                    at = pl.multiple_of(start * heads, LANES * heads)
                    values[pl.ds(at, LANES * heads), :] = rows

                expand(
                    block, slabs, blk, per_unit, heads, rotary, gain, key_w, value_w, mixed,
                    put_keys, put_values,
                )

    def own(i):
        q = source(c, i, seqs)
        arrived(g, q)

        @pl.when(above & (g == 0))
        def _():
            relay(g, q, g + 1).start()

        @pl.when(below & (g == planes - 1))
        def _():
            relay(g, q, g - 1).start()

    @pl.loop(1, seqs)
    def _(i):
        pl.when(g == planes - 1)(lambda: own(i))
        pl.when((g < planes - 1) | (g == 0))(lambda: pass_mid(1, i))
        pl.when((g == 0) & above)(lambda: own(i))

    @pl.loop(1, seqs)
    def _(i):
        pl.when((g == planes - 1) & below)(lambda: pass_mid(1, i))

    pl.when(inner(1, 1) & below)(lambda: own_along(g - 1).start())
    pl.when(inner(0, 1) & above)(lambda: own_along(g + 1).start())
    pl.when(jnp.logical_not(edge))(lambda: along(1))

    @pl.when(jnp.logical_not(edge))
    def _():
        settle(c, 1, 1)

        @pl.loop(1, seqs)
        def _(i):
            take(1, i, True)

    @pl.loop(1, seqs + 1)
    def _(i):
        @pl.when(i < seqs)
        def _():
            pass_mid(2, i)
            pl.when(jnp.logical_not(edge))(lambda: own(i))
            pl.when(edge)(lambda: take(1, i))
            pl.when(jnp.logical_not(edge))(lambda: take(1, i, False))

        @pl.when((i == seqs) & edge)
        def _():
            along(1)

        @pl.when((i < seqs) | edge)
        def _():
            settle(jnp.where(i == seqs, c, source(c, i, seqs)), 1, 1)

    along(2)

    def origin(i):
        return jnp.where(i == 0, c, source(c, jnp.maximum(i, 0), seqs))

    @pl.loop(2, max(planes, 3))
    def _(far):
        turn = gate & (far == planes - 2)

        @pl.loop(0, seqs + 1)
        def _(i):
            @pl.when((i == 0) & (far > 2))
            def _():
                along(far)

            @pl.when(turn & (ens == 1) & (i == max(seqs - HELD, 1)))
            def _():
                pl.semaphore_wait(ready.at[1], 1)

            @pl.when((i > 0) & (i < seqs))
            def _():
                take(far, i)

            at = jnp.where(edge, i, i - 1)

            @pl.when((at >= 0) & (at < seqs))
            def _():
                settle(origin(at), far, far)

            @pl.when(turn & (ens == 0) & (i == seqs - 1))
            def _():
                pl.semaphore_signal(ready.at[1], inc=1, device_id={"ens": 1}, device_id_type=MESH)

    last[...] = raw[end_q, pl.ds(end_u * per_unit, per_unit)]

    ups, downs = jnp.minimum(planes - 1 - g, 1), jnp.minimum(g, 1)
    total = seqs * (ups + downs + g * ups + (planes - 1 - g) * downs)
    spread = sum(jnp.where(inner(way, far), 1, 0) for way in (0, 1) for far in (1, 2))
    total = total + (seqs - 1) * (1 + spread)
    near, next_near = jnp.where(inner(1, 1) & below, 1, 0), jnp.where(inner(1, 2), 1, 0)
    parts = jnp.where(c == 0, (seqs - 1) * (near + next_near), 0)
    if not give:
        parts = 0 * parts

    @pl.loop(0, total - parts)
    def _(_):
        own_along(g).wait_send()

    @pl.loop(0, parts)
    def _(_):
        forward(1, 1, kept, g).wait_send()

    if give:
        @pl.when((c > 0) & (near > 0))
        def _():
            relay_given(g, c, g).wait_send()


def store(
    seqs, planes, heads, rotary, blk,
    keys, values, last, key_w, value_w, gain,
    keys_out, values_out,
    end_keys, end_values, mixed, sems,
):
    c, g = lax.axis_index("ctx"), lax.axis_index("group")
    slabs = gain.shape[1] // LANES
    per_unit = LANES // blk
    units = planes // per_unit
    key_part = key_w.shape[0] // heads
    blocks = seqs * units
    end_q, end_u = pending(c, g, seqs, planes, units)
    end = end_q * units + end_u

    def columns(b):
        return pl.ds(pl.multiple_of(b * LANES, LANES), LANES)

    def rows(b):
        return pl.ds(pl.multiple_of(b * LANES * heads, LANES * heads), LANES * heads)

    @pl.loop(1, blocks)
    def _(j):
        b = lax.rem(end + j, blocks)
        pltpu.make_async_copy(
            keys.at[:, :, columns(b)], keys_out.at[:, :, columns(b)], sems.at[0]
        ).start()
        pltpu.make_async_copy(values.at[rows(b)], values_out.at[rows(b)], sems.at[1]).start()

    def block(row, count):
        return last[:, row : row + count, :]

    def put_keys(h, wide_keys, turned):
        end_keys[h, :key_part, :] = wide_keys
        end_keys[h, key_part:, :] = turned

    def put_values(part):
        end_values[...] = part

    expand(
        block, slabs, blk, per_unit, heads, rotary, gain, key_w, value_w, mixed,
        put_keys, put_values,
    )
    pltpu.make_async_copy(end_keys, keys_out.at[:, :, columns(end)], sems.at[0]).start()
    pltpu.make_async_copy(end_values, values_out.at[rows(end)], sems.at[1]).start()
    pltpu.make_async_copy(keys, keys_out, sems.at[0]).wait()
    pltpu.make_async_copy(values, values_out, sems.at[1]).wait()


def per_device(latents, rotary_rows, latent_gain, key_up, value_up):
    seqs, planes = lax.axis_size("ctx"), lax.axis_size("group")
    _, blk, latent = latents.shape
    rotary = rotary_rows.shape[2]
    heads, key_part = key_up.shape[1:]
    size = value_up.shape[2]
    length = seqs * planes * blk
    per_unit = LANES // blk
    ways = 1 if planes <= 4 else 2
    packed = (blk * (latent + rotary) // LANES, LANES)
    dma = pltpu.SemaphoreType.DMA
    in_hbm = functools.partial(pltpu.with_memory_space_constraint, memory_space=pltpu.HBM)
    outer = pl.BlockSpec(memory_space=pltpu.HBM)
    inside = pl.BlockSpec(memory_space=pltpu.VMEM)
    held = pl.pallas_call(
        functools.partial(kernel, seqs, planes, heads, rotary),
        out_shape=(
            pltpu.VMEM((heads, key_part + rotary, length), BF16),
            pltpu.VMEM((length * heads, size), BF16),
            pltpu.VMEM((per_unit, *packed), BF16),
            pltpu.VMEM((heads * key_part, latent), BF16),
            pltpu.VMEM((latent, heads * size), BF16),
            pltpu.VMEM((1, latent), jnp.float32),
        ),
        in_specs=[outer] * 5,
        out_specs=(inside,) * 6,
        scratch_shapes=[
            pltpu.VMEM((seqs, *packed), BF16),
            pltpu.VMEM((seqs, planes, *packed), BF16),
            pltpu.VMEM((ways, 2, seqs - 1, *packed), BF16),
            pltpu.VMEM((seqs, blk, rotary), BF16),
            pltpu.VMEM((latent * heads, key_part), BF16),
            pltpu.VMEM((latent * heads, size), BF16),
            pltpu.VMEM((latent * heads, size), jnp.float32),
            pltpu.VMEM((LANES * heads, size), jnp.float32),
            dma((4,)),
            dma((planes, seqs)),
            dma((ways, 2, seqs - 1)),
            dma,
            pltpu.SemaphoreType.REGULAR((2 + seqs,)),
        ],
        compiler_params=pltpu.CompilerParams(
            collective_id=0, has_side_effects=True, vmem_limit_bytes=32 * 1024 * 1024
        ),
    )(
        in_hbm(latents),
        in_hbm(rotary_rows),
        in_hbm(latent_gain.reshape(1, latent)),
        in_hbm(key_up.reshape(latent * heads, key_part)),
        in_hbm(value_up.reshape(latent * heads, size)),
    )
    keys, values = pl.pallas_call(
        functools.partial(store, seqs, planes, heads, rotary, blk),
        out_shape=(
            jax.ShapeDtypeStruct((heads, key_part + rotary, length), BF16),
            jax.ShapeDtypeStruct((length * heads, size), BF16),
        ),
        in_specs=[inside] * 6,
        out_specs=(outer, outer),
        scratch_shapes=[
            pltpu.VMEM((heads, key_part + rotary, LANES), BF16),
            pltpu.VMEM((LANES * heads, size), BF16),
            pltpu.VMEM((LANES * heads, size), jnp.float32),
            dma((2,)),
        ],
        compiler_params=pltpu.CompilerParams(vmem_limit_bytes=16 * 1024 * 1024),
    )(*held)
    return keys[None], values.reshape(1, length, heads, size)


def solution(mesh):
    in_specs = (
        P("ens", ("ctx", "group"), None),
        P("ens", ("ctx", "group"), None),
        P(),
        P("ens", "group", None),
        P("ens", "group", None),
    )
    out_specs = (P(("ens", "ctx"), "group", None, None), P(("ens", "ctx"), None, "group", None))
    return jax.shard_map(
        per_device, mesh=mesh, in_specs=in_specs, out_specs=out_specs, check_vma=False
    )
```

```python
import functools

import jax
import jax.numpy as jnp
from jax import lax
from jax.experimental import pallas as pl
from jax.experimental.pallas import tpu as pltpu
from jax.sharding import PartitionSpec as P

MESH = pl.DeviceIdType.MESH
LANES = 128
BF16 = jnp.bfloat16
GIVEN = 3, 18
HELD, HELD_FIRST = 2, 1


def xor(me, step, count):
    total, bit = 0, 1
    while bit < count:
        total = total + bit * lax.rem(me // bit + step // bit, 2)
        bit *= 2
    return total


def partner(me, step, count):
    return lax.rem(me + step, count) if count & (count - 1) else xor(me, step, count)


def source(me, step, count):
    return lax.rem(me + count - step, count) if count & (count - 1) else xor(me, step, count)


def join(a, b, count):
    if count & (count - 1):
        return jnp.maximum(a, b)
    total, bit = 0, 1
    while bit < count:
        total = total + bit * jnp.maximum(lax.rem(a // bit, 2), lax.rem(b // bit, 2))
        bit *= 2
    return total


def lower(c, count):
    if count & (count - 1):
        return c
    total, bit = 1, 1
    while bit < count:
        total = total * (1 + lax.rem(c // bit, 2))
        bit *= 2
    return total - 1


def pending(c, g, seqs, planes, units):
    q = source(c, seqs - 1, seqs) if seqs > 1 else c
    return q, jnp.where(2 * g < planes, units - 1, 0)


def expand(block, slabs, blk, per_unit, heads, rotary, gain, key_w, value_w, mixed, put_keys, put_values):
    key_part = key_w.shape[0] // heads
    size = value_w.shape[1] // heads
    x = jnp.concatenate(
        [block(k * blk, blk).astype(jnp.float32).reshape(LANES, LANES) for k in range(slabs)],
        axis=1,
    )
    mean = jnp.mean(x * x, axis=-1, keepdims=True)
    rows = (x * lax.rsqrt(mean + 1e-06) * gain[...]).astype(BF16)
    wide_keys = lax.dot_general(
        key_w[...], rows, (((1,), (1,)), ((), ())), preferred_element_type=jnp.float32
    ).astype(BF16)
    tails = block(slabs * blk, blk * rotary // LANES).astype(jnp.float32)
    pieces = []
    for j in range(per_unit):
        pieces += [tails[j][:, :rotary], pltpu.roll(tails[j], rotary, 1)[:, :rotary]]
    turned = jnp.concatenate(pieces, axis=0).T.astype(BF16)
    for h in range(heads):
        put_keys(h, wide_keys[h * key_part : (h + 1) * key_part], turned)
    wide_values = jnp.dot(rows, value_w[...], preferred_element_type=jnp.float32)
    for h in range(heads):
        mixed[pl.ds(h, LANES, stride=heads), :] = wide_values[:, h * size : (h + 1) * size]
    put_values(mixed[...].astype(BF16))


def kernel(
    seqs, planes, heads, rotary,
    lat, rot, gain_in, key_up, value_up,
    keys, values, last, key_w, value_w, gain,
    stage, raw, mid, rot_stage, key_stage, value_stage, wide, mixed,
    load_sem, got, mid_got, sent, ready,
):
    ens, c, g = lax.axis_index("ens"), lax.axis_index("ctx"), lax.axis_index("group")
    blk, latent = lat.shape[1:]
    slabs = latent // LANES
    tail = slabs * blk
    half = blk // 2
    give = stage.shape[1] // 16 * GIVEN[0] // GIVEN[1] * 16
    keep = stage.shape[1] - give
    kept, given = pl.ds(0, keep), pl.ds(keep, give)
    ways = mid.shape[0]
    per_unit = LANES // blk
    units = planes // per_unit
    key_part = key_w.shape[0] // heads
    size = value_w.shape[1] // heads
    first = partner(c, 1, seqs)

    def lat_load(s, k, sem):
        return pltpu.make_async_copy(
            lat.at[s, :, pl.ds(k * LANES, LANES)],
            stage.at[s, pl.ds(k * blk, blk), :],
            load_sem.at[sem],
        )

    rot_load = pltpu.make_async_copy(rot, rot_stage, load_sem.at[0])
    for k in range(slabs):
        lat_load(first, k, 1).start()
    rot_load.start()

    @pl.loop(1, seqs)
    def _(b):
        for k in range(slabs):
            lat_load(partner(first, b, seqs), k, 0).start()

    loads = [
        pltpu.make_async_copy(key_up, key_stage, load_sem.at[2]),
        pltpu.make_async_copy(value_up, value_stage, load_sem.at[2]),
        pltpu.make_async_copy(gain_in, gain, load_sem.at[2]),
    ]
    for load in loads:
        load.start()

    barrier = pltpu.get_barrier_semaphore()
    above, below = g < planes - 1, g > 0
    edge = (g == 0) | (g == planes - 1)
    gate = (g == 1) | (g == planes - 2) if planes > 3 else g < 0

    def inner(way, far):
        return g > far if way == 0 else g + far < planes - 1

    @pl.when(above)
    def _():
        pl.semaphore_signal(barrier, inc=1, device_id={"group": g + 1}, device_id_type=MESH)

    @pl.when(gate & (ens == 1))
    def _():
        pl.semaphore_signal(barrier, inc=1, device_id={"ens": 0}, device_id_type=MESH)

    @pl.loop(c + 1, seqs)
    def _(s):
        @pl.when(join(c, s, seqs) == s)
        def _():
            pl.semaphore_signal(barrier, inc=1, device_id={"ctx": s}, device_id_type=MESH)

    def remote(src, dst, in_sem, to):
        return pltpu.make_async_remote_copy(
            src_ref=src, dst_ref=dst, send_sem=sent, recv_sem=in_sem,
            device_id=to, device_id_type=MESH,
        )

    def out(way, i, s, part, to):
        return remote(
            stage.at[s, part], mid.at[way % ways, 0, i - 1, part], mid_got.at[way % ways, 0, i - 1], {"group": to}
        )

    def own_along(to):
        return remote(stage.at[c], raw.at[c, g], got.at[g, c], {"group": to})

    def own_side(s):
        return remote(stage.at[s], raw.at[c, g], got.at[g, c], {"ctx": s})

    def forward(way, i, part, to):
        return remote(
            mid.at[way % ways, 0, i - 1, part], mid.at[way % ways, 1, i - 1, part],
            mid_got.at[way % ways, 1, i - 1], {"group": to},
        )

    def scatter(way, far, i, part, p, s):
        return remote(mid.at[way % ways, far, i - 1, part], raw.at[c, p, part], got.at[p, c], {"ctx": s})

    def relay(p, q, to):
        return remote(raw.at[q, p], raw.at[q, p], got.at[p, q], {"group": to})

    def relay_given(p, q, to):
        return remote(raw.at[q, p, given], raw.at[q, p, given], got.at[p, q], {"group": to})

    whole = pl.ds(0, stage.shape[1])
    wide_part, rot_part = pl.ds(0, tail), pl.ds(tail, half)

    def rest(way, to):
        @pl.loop(2, seqs)
        def _(i):
            out(way, i, partner(c, i, seqs), whole, to).start()

    early = lower(c, seqs) + jnp.minimum(g, 1) + jnp.where(gate & (ens == 0), 1, 0)

    @pl.when(early > 0)
    def _():
        pl.semaphore_wait(barrier, early)

    @pl.when(below)
    def _():
        pl.semaphore_signal(ready.at[0], inc=1, device_id={"group": g - 1}, device_id_type=MESH)

    @pl.loop(0, c)
    def _(s):
        @pl.when(join(c, s, seqs) == c)
        def _():
            pl.semaphore_signal(ready.at[1 + c], inc=1, device_id={"ctx": s}, device_id_type=MESH)

    def prepare():
        for load in loads:
            load.wait()
        wide[...] = key_stage[...].astype(jnp.float32)
        for h in range(heads):
            key_w[h * key_part : (h + 1) * key_part, :] = (
                wide[pl.ds(h, latent, stride=heads), :].T.astype(BF16)
            )
        wide[...] = value_stage[...].astype(jnp.float32)
        for h in range(heads):
            value_w[:, h * size : (h + 1) * size] = (
                wide[pl.ds(h, latent, stride=heads), :].astype(BF16)
            )

    for k in range(slabs):
        lat_load(first, k, 1).wait()

    @pl.when(below & above)
    def _():
        out(1, 1, first, wide_part, g - 1).start()

    @pl.loop(1, seqs)
    def _(b):
        for k in range(slabs):
            lat_load(partner(first, b, seqs), k, 0).wait()

    rot_load.wait()

    @pl.loop(0, seqs)
    def _(s):
        block = rot_stage[s].astype(jnp.float32)
        both = jnp.concatenate([block[:half], block[half:]], axis=1)
        stage[s, pl.ds(tail, half), :] = both.astype(BF16)

    @pl.when(below & above)
    def _():
        out(1, 1, first, rot_part, g - 1).start()
        rest(1, g - 1)
        pl.when(jnp.logical_not(inner(1, 1)))(lambda: own_along(g - 1).start())
        pl.semaphore_wait(ready.at[0], 1)
        out(0, 1, first, whole, g + 1).start()
        rest(0, g + 1)
        pl.when(jnp.logical_not(inner(0, 1)))(lambda: own_along(g + 1).start())

    @pl.when(below & (g == planes - 1))
    def _():
        own_along(g - 1).start()

    @pl.when(above & (g == 0))
    def _():
        pl.semaphore_wait(ready.at[0], 1)
        own_along(g + 1).start()

    @pl.loop(c, seqs)
    def _(t):
        @pl.when(join(c, t, seqs) == t)
        def _():
            @pl.when(t > c)
            def _():
                pl.semaphore_wait(ready.at[1 + t], 1)

            @pl.loop(1, seqs)
            def _(i):
                s = partner(c, i, seqs)

                @pl.when(join(c, s, seqs) == t)
                def _():
                    own_side(s).start()

    raw[c, g] = stage[c]
    prepare()

    low = 2 * g < planes

    def near_first(go):
        pl.when(low)(lambda: go(1))
        go(0)
        pl.when(jnp.logical_not(low))(lambda: go(1))

    def arrived(p, q):
        relay(p, q, g).wait_recv()

    def plane(way, far):
        return g - far if way == 0 else g + far

    def exists(way, far):
        return g >= far if way == 0 else g + far < planes

    def onward(way):
        return above if way == 0 else below

    def towards(way):
        return g + 1 if way == 0 else g - 1

    def along(far):
        def go(way):
            @pl.when(exists(way, far))
            def _():
                arrived(plane(way, far), c)

                @pl.when(onward(way))
                def _():
                    relay(plane(way, far), c, towards(way)).start()

        near_first(go)

    def sized(way, go):
        if way == 0 or not give:
            go(whole)
        else:
            pl.when(c > 0)(lambda: go(whole))
            pl.when(c == 0)(lambda: go(kept))

    def pass_mid(far, i):
        def go(way):
            s = partner(c, i, seqs)

            @pl.when(inner(way, far))
            def _():
                if far == 1:
                    out(way, i, c, whole, g).wait_recv()
                    scatter(way, 0, i, whole, plane(way, far), s).start()

                    @pl.when(onward(way))
                    def _():
                        sized(way, lambda part: forward(way, i, part, towards(way)).start())
                else:
                    def onto(part):
                        forward(way, i, part, g).wait_recv()
                        scatter(way, 1, i, part, plane(way, far), s).start()

                    sized(way, onto)

        near_first(go)

    def take(far, i, chain=None):
        def go(way):
            wanted = exists(way, far)
            if chain is not None:
                wanted = wanted & (inner(way, far) != chain)

            @pl.when(wanted)
            def _():
                q = source(c, i, seqs)
                arrived(plane(way, far), q)

                @pl.when(onward(way) & ((far > 1) | jnp.logical_not(inner(way, 1))))
                def _():
                    relay(plane(way, far), q, towards(way)).start()

                if way == 1 and give:
                    @pl.when(below & inner(1, 1) & (far == 1) & (q == 0))
                    def _():
                        relay_given(plane(way, far), q, g - 1).start()

        near_first(go)

    end_q, end_u = pending(c, g, seqs, planes, units)

    def settle(q, low_far, high_far):
        @pl.loop(0, units)
        def _(u):
            far = jnp.maximum(g - u * per_unit, (u + 1) * per_unit - 1 - g)
            far = jnp.maximum(far, 1)
            wanted = (far >= low_far) & (far <= high_far)

            @pl.when(wanted & ((q != end_q) | (u != end_u)))
            def _():
                begin = u * per_unit
                start = pl.multiple_of((q * planes + begin) * blk, LANES)

                def block(row, count):
                    return raw[q, pl.ds(begin, per_unit), row : row + count, :]

                def put_keys(h, wide_keys, turned):
                    keys[h, :key_part, pl.ds(start, LANES)] = wide_keys
                    keys[h, key_part:, pl.ds(start, LANES)] = turned

                def put_values(rows):
                    at = pl.multiple_of(start * heads, LANES * heads)
                    values[pl.ds(at, LANES * heads), :] = rows

                expand(
                    block, slabs, blk, per_unit, heads, rotary, gain, key_w, value_w, mixed,
                    put_keys, put_values,
                )

    def own(i):
        q = source(c, i, seqs)
        arrived(g, q)

        @pl.when(above & (g == 0))
        def _():
            relay(g, q, g + 1).start()

        @pl.when(below & (g == planes - 1))
        def _():
            relay(g, q, g - 1).start()

    @pl.loop(1, seqs)
    def _(i):
        pl.when(g == planes - 1)(lambda: own(i))
        pl.when((g < planes - 1) | (g == 0))(lambda: pass_mid(1, i))
        pl.when((g == 0) & above)(lambda: own(i))

    @pl.loop(1, seqs)
    def _(i):
        pl.when((g == planes - 1) & below)(lambda: pass_mid(1, i))

    pl.when(inner(1, 1) & below)(lambda: own_along(g - 1).start())
    pl.when(inner(0, 1) & above)(lambda: own_along(g + 1).start())
    pl.when(jnp.logical_not(edge))(lambda: along(1))

    @pl.when(jnp.logical_not(edge))
    def _():
        settle(c, 1, 1)

        @pl.loop(1, seqs)
        def _(i):
            take(1, i, True)

    @pl.loop(1, seqs + 1)
    def _(i):
        @pl.when(i < seqs)
        def _():
            pass_mid(2, i)
            pl.when(jnp.logical_not(edge))(lambda: own(i))
            pl.when(edge)(lambda: take(1, i))
            pl.when(jnp.logical_not(edge))(lambda: take(1, i, False))

        @pl.when((i == seqs) & edge)
        def _():
            along(1)

        @pl.when((i < seqs) | edge)
        def _():
            settle(jnp.where(i == seqs, c, source(c, i, seqs)), 1, 1)

    along(2)

    def drain():
        ups, downs = jnp.minimum(planes - 1 - g, 1), jnp.minimum(g, 1)
        total = seqs * (ups + downs + g * ups + (planes - 1 - g) * downs)
        spread = sum(jnp.where(inner(way, far), 1, 0) for way in (0, 1) for far in (1, 2))
        total = total + (seqs - 1) * (1 + spread)
        near, next_near = jnp.where(inner(1, 1) & below, 1, 0), jnp.where(inner(1, 2), 1, 0)
        parts = jnp.where(c == 0, (seqs - 1) * (near + next_near), 0)
        if not give:
            parts = 0 * parts

        @pl.loop(0, total - parts)
        def _(_):
            own_along(g).wait_send()

        @pl.loop(0, parts)
        def _(_):
            forward(1, 1, kept, g).wait_send()

        if give:
            @pl.when((c > 0) & (near > 0))
            def _():
                relay_given(g, c, g).wait_send()

    pl.when(edge)(drain)

    def origin(i):
        return jnp.where(i == 0, c, source(c, jnp.maximum(i, 0), seqs))

    @pl.loop(2, max(planes, 3))
    def _(far):
        turn = gate & (far == planes - 2)

        @pl.loop(0, seqs + 1)
        def _(i):
            @pl.when((i == 0) & (far > 2))
            def _():
                along(far)

            @pl.when(turn & (ens == 1) & (i == jnp.where(c == 0, seqs - HELD_FIRST, max(seqs - HELD, 1))))
            def _():
                pl.semaphore_wait(ready.at[1], 1)

            at = jnp.where(edge, i, i - 1)
            late = turn & (ens == 1) & (i == seqs - 1) & (c == 0)
            pl.when(late)(lambda: settle(origin(at), far, far))

            @pl.when((i > 0) & (i < seqs))
            def _():
                take(far, i)

            done = turn & (ens == 0) & (i == seqs - 1)

            def release():
                pl.semaphore_signal(ready.at[1], inc=1, device_id={"ens": 1}, device_id_type=MESH)

            pl.when(done & (c > 0))(release)

            @pl.when((at >= 0) & (at < seqs) & jnp.logical_not(late))
            def _():
                settle(origin(at), far, far)

            pl.when(done & (c == 0))(release)

    last[...] = raw[end_q, pl.ds(end_u * per_unit, per_unit)]

    pl.when(jnp.logical_not(edge))(drain)


def store(
    seqs, planes, heads, rotary, blk,
    keys, values, last, key_w, value_w, gain,
    keys_out, values_out,
    end_keys, end_values, mixed, sems,
):
    c, g = lax.axis_index("ctx"), lax.axis_index("group")
    slabs = gain.shape[1] // LANES
    per_unit = LANES // blk
    units = planes // per_unit
    key_part = key_w.shape[0] // heads
    blocks = seqs * units
    end_q, end_u = pending(c, g, seqs, planes, units)
    end = end_q * units + end_u

    def columns(b):
        return pl.ds(pl.multiple_of(b * LANES, LANES), LANES)

    def rows(b):
        return pl.ds(pl.multiple_of(b * LANES * heads, LANES * heads), LANES * heads)

    @pl.loop(1, blocks)
    def _(j):
        b = lax.rem(end + j, blocks)
        pltpu.make_async_copy(
            keys.at[:, :, columns(b)], keys_out.at[:, :, columns(b)], sems.at[0]
        ).start()
        pltpu.make_async_copy(values.at[rows(b)], values_out.at[rows(b)], sems.at[1]).start()

    def block(row, count):
        return last[:, row : row + count, :]

    def put_keys(h, wide_keys, turned):
        end_keys[h, :key_part, :] = wide_keys
        end_keys[h, key_part:, :] = turned

    def put_values(part):
        end_values[...] = part

    expand(
        block, slabs, blk, per_unit, heads, rotary, gain, key_w, value_w, mixed,
        put_keys, put_values,
    )
    pltpu.make_async_copy(end_keys, keys_out.at[:, :, columns(end)], sems.at[0]).start()
    pltpu.make_async_copy(end_values, values_out.at[rows(end)], sems.at[1]).start()
    pltpu.make_async_copy(keys, keys_out, sems.at[0]).wait()
    pltpu.make_async_copy(values, values_out, sems.at[1]).wait()


def per_device(latents, rotary_rows, latent_gain, key_up, value_up):
    seqs, planes = lax.axis_size("ctx"), lax.axis_size("group")
    _, blk, latent = latents.shape
    rotary = rotary_rows.shape[2]
    heads, key_part = key_up.shape[1:]
    size = value_up.shape[2]
    length = seqs * planes * blk
    per_unit = LANES // blk
    ways = 1 if planes <= 4 else 2
    packed = (blk * (latent + rotary) // LANES, LANES)
    dma = pltpu.SemaphoreType.DMA
    in_hbm = functools.partial(pltpu.with_memory_space_constraint, memory_space=pltpu.HBM)
    outer = pl.BlockSpec(memory_space=pltpu.HBM)
    inside = pl.BlockSpec(memory_space=pltpu.VMEM)
    held = pl.pallas_call(
        functools.partial(kernel, seqs, planes, heads, rotary),
        out_shape=(
            pltpu.VMEM((heads, key_part + rotary, length), BF16),
            pltpu.VMEM((length * heads, size), BF16),
            pltpu.VMEM((per_unit, *packed), BF16),
            pltpu.VMEM((heads * key_part, latent), BF16),
            pltpu.VMEM((latent, heads * size), BF16),
            pltpu.VMEM((1, latent), jnp.float32),
        ),
        in_specs=[outer] * 5,
        out_specs=(inside,) * 6,
        scratch_shapes=[
            pltpu.VMEM((seqs, *packed), BF16),
            pltpu.VMEM((seqs, planes, *packed), BF16),
            pltpu.VMEM((ways, 2, seqs - 1, *packed), BF16),
            pltpu.VMEM((seqs, blk, rotary), BF16),
            pltpu.VMEM((latent * heads, key_part), BF16),
            pltpu.VMEM((latent * heads, size), BF16),
            pltpu.VMEM((latent * heads, size), jnp.float32),
            pltpu.VMEM((LANES * heads, size), jnp.float32),
            dma((3,)),
            dma((planes, seqs)),
            dma((ways, 2, seqs - 1)),
            dma,
            pltpu.SemaphoreType.REGULAR((1 + seqs,)),
        ],
        compiler_params=pltpu.CompilerParams(
            collective_id=0, has_side_effects=True, vmem_limit_bytes=32 * 1024 * 1024
        ),
    )(
        in_hbm(latents),
        in_hbm(rotary_rows),
        in_hbm(latent_gain.reshape(1, latent)),
        in_hbm(key_up.reshape(latent * heads, key_part)),
        in_hbm(value_up.reshape(latent * heads, size)),
    )
    keys, values = pl.pallas_call(
        functools.partial(store, seqs, planes, heads, rotary, blk),
        out_shape=(
            jax.ShapeDtypeStruct((heads, key_part + rotary, length), BF16),
            jax.ShapeDtypeStruct((length * heads, size), BF16),
        ),
        in_specs=[inside] * 6,
        out_specs=(outer, outer),
        scratch_shapes=[
            pltpu.VMEM((heads, key_part + rotary, LANES), BF16),
            pltpu.VMEM((LANES * heads, size), BF16),
            pltpu.VMEM((LANES * heads, size), jnp.float32),
            dma((2,)),
        ],
        compiler_params=pltpu.CompilerParams(vmem_limit_bytes=16 * 1024 * 1024),
    )(*held)
    return keys[None], values.reshape(1, length, heads, size)


def solution(mesh):
    in_specs = (
        P("ens", ("ctx", "group"), None),
        P("ens", ("ctx", "group"), None),
        P(),
        P("ens", "group", None),
        P("ens", "group", None),
    )
    out_specs = (P(("ens", "ctx"), "group", None, None), P(("ens", "ctx"), None, "group", None))
    return jax.shard_map(
        per_device, mesh=mesh, in_specs=in_specs, out_specs=out_specs, check_vma=False
    )
```

```python
import functools

import jax
import jax.numpy as jnp
from jax import lax
from jax.experimental import pallas as pl
from jax.experimental.pallas import tpu as pltpu
from jax.sharding import PartitionSpec as P

MESH = pl.DeviceIdType.MESH
LANES = 128
BF16 = jnp.bfloat16
GIVEN = 3, 18
HELD = 1


def xor(me, step, count):
    total, bit = 0, 1
    while bit < count:
        total = total + bit * lax.rem(me // bit + step // bit, 2)
        bit *= 2
    return total


def partner(me, step, count):
    return lax.rem(me + step, count) if count & (count - 1) else xor(me, step, count)


def source(me, step, count):
    return lax.rem(me + count - step, count) if count & (count - 1) else xor(me, step, count)


def join(a, b, count):
    if count & (count - 1):
        return jnp.maximum(a, b)
    total, bit = 0, 1
    while bit < count:
        total = total + bit * jnp.maximum(lax.rem(a // bit, 2), lax.rem(b // bit, 2))
        bit *= 2
    return total


def lower(c, count):
    if count & (count - 1):
        return c
    total, bit = 1, 1
    while bit < count:
        total = total * (1 + lax.rem(c // bit, 2))
        bit *= 2
    return total - 1


def pending(c, g, seqs, planes, units):
    q = source(c, seqs - 1, seqs) if seqs > 1 else c
    return q, jnp.where(2 * g < planes, units - 1, 0)


def expand(block, slabs, blk, per_unit, heads, rotary, gain, key_w, value_w, mixed, put_keys, put_values):
    key_part = key_w.shape[0] // heads
    size = value_w.shape[1] // heads
    x = jnp.concatenate(
        [block(k * blk, blk).astype(jnp.float32).reshape(LANES, LANES) for k in range(slabs)],
        axis=1,
    )
    mean = jnp.mean(x * x, axis=-1, keepdims=True)
    rows = (x * lax.rsqrt(mean + 1e-06) * gain[...]).astype(BF16)
    wide_keys = lax.dot_general(
        key_w[...], rows, (((1,), (1,)), ((), ())), preferred_element_type=jnp.float32
    ).astype(BF16)
    tails = block(slabs * blk, blk * rotary // LANES).astype(jnp.float32)
    pieces = []
    for j in range(per_unit):
        pieces += [tails[j][:, :rotary], pltpu.roll(tails[j], rotary, 1)[:, :rotary]]
    turned = jnp.concatenate(pieces, axis=0).T.astype(BF16)
    for h in range(heads):
        put_keys(h, wide_keys[h * key_part : (h + 1) * key_part], turned)
    wide_values = jnp.dot(rows, value_w[...], preferred_element_type=jnp.float32)
    for h in range(heads):
        mixed[pl.ds(h, LANES, stride=heads), :] = wide_values[:, h * size : (h + 1) * size]
    put_values(mixed[...].astype(BF16))


def kernel(
    seqs, planes, heads, rotary,
    lat, rot, gain_in, key_up, value_up,
    keys, values, last, key_w, value_w, gain,
    stage, raw, mid, rot_stage, key_stage, value_stage, wide, mixed,
    load_sem, got, mid_got, sent, ready,
):
    ens, c, g = lax.axis_index("ens"), lax.axis_index("ctx"), lax.axis_index("group")
    blk, latent = lat.shape[1:]
    slabs = latent // LANES
    tail = slabs * blk
    half = blk // 2
    give = stage.shape[1] // 16 * GIVEN[0] // GIVEN[1] * 16
    keep = stage.shape[1] - give
    kept, given = pl.ds(0, keep), pl.ds(keep, give)
    ways = mid.shape[0]
    per_unit = LANES // blk
    units = planes // per_unit
    key_part = key_w.shape[0] // heads
    size = value_w.shape[1] // heads
    first = partner(c, 1, seqs)

    def lat_load(s, k, sem):
        return pltpu.make_async_copy(
            lat.at[s, :, pl.ds(k * LANES, LANES)],
            stage.at[s, pl.ds(k * blk, blk), :],
            load_sem.at[sem],
        )

    rot_load = pltpu.make_async_copy(rot, rot_stage, load_sem.at[0])
    for k in range(slabs):
        lat_load(first, k, 1).start()
    rot_load.start()

    @pl.loop(1, seqs)
    def _(b):
        for k in range(slabs):
            lat_load(partner(first, b, seqs), k, 0).start()

    loads = [
        pltpu.make_async_copy(key_up, key_stage, load_sem.at[2]),
        pltpu.make_async_copy(value_up, value_stage, load_sem.at[2]),
        pltpu.make_async_copy(gain_in, gain, load_sem.at[2]),
    ]
    for load in loads:
        load.start()

    barrier = pltpu.get_barrier_semaphore()
    above, below = g < planes - 1, g > 0
    edge = (g == 0) | (g == planes - 1)
    gate = (g == 1) | (g == planes - 2) if planes > 3 else g < 0

    def inner(way, far):
        return g > far if way == 0 else g + far < planes - 1

    @pl.when(above)
    def _():
        pl.semaphore_signal(barrier, inc=1, device_id={"group": g + 1}, device_id_type=MESH)

    @pl.when(gate & (ens == 1))
    def _():
        pl.semaphore_signal(barrier, inc=1, device_id={"ens": 0}, device_id_type=MESH)

    @pl.loop(c + 1, seqs)
    def _(s):
        @pl.when(join(c, s, seqs) == s)
        def _():
            pl.semaphore_signal(barrier, inc=1, device_id={"ctx": s}, device_id_type=MESH)

    def remote(src, dst, in_sem, to):
        return pltpu.make_async_remote_copy(
            src_ref=src, dst_ref=dst, send_sem=sent, recv_sem=in_sem,
            device_id=to, device_id_type=MESH,
        )

    def out(way, i, s, part, to):
        return remote(
            stage.at[s, part], mid.at[way % ways, 0, i - 1, part], mid_got.at[way % ways, 0, i - 1], {"group": to}
        )

    def own_along(to):
        return remote(stage.at[c], raw.at[c, g], got.at[g, c], {"group": to})

    def own_side(s):
        return remote(stage.at[s], raw.at[c, g], got.at[g, c], {"ctx": s})

    def forward(way, i, part, to):
        return remote(
            mid.at[way % ways, 0, i - 1, part], mid.at[way % ways, 1, i - 1, part],
            mid_got.at[way % ways, 1, i - 1], {"group": to},
        )

    def scatter(way, far, i, part, p, s):
        return remote(mid.at[way % ways, far, i - 1, part], raw.at[c, p, part], got.at[p, c], {"ctx": s})

    def relay(p, q, to):
        return remote(raw.at[q, p], raw.at[q, p], got.at[p, q], {"group": to})

    def relay_given(p, q, to):
        return remote(raw.at[q, p, given], raw.at[q, p, given], got.at[p, q], {"group": to})

    whole = pl.ds(0, stage.shape[1])
    wide_part, rot_part = pl.ds(0, tail), pl.ds(tail, half)

    def rest(way, to):
        @pl.loop(2, seqs)
        def _(i):
            out(way, i, partner(c, i, seqs), whole, to).start()

    early = lower(c, seqs) + jnp.minimum(g, 1) + jnp.where(gate & (ens == 0), 1, 0)

    @pl.when(early > 0)
    def _():
        pl.semaphore_wait(barrier, early)

    @pl.when(below)
    def _():
        pl.semaphore_signal(ready.at[0], inc=1, device_id={"group": g - 1}, device_id_type=MESH)

    @pl.loop(0, c)
    def _(s):
        @pl.when(join(c, s, seqs) == c)
        def _():
            pl.semaphore_signal(ready.at[1 + c], inc=1, device_id={"ctx": s}, device_id_type=MESH)

    def prepare():
        for load in loads:
            load.wait()
        wide[...] = key_stage[...].astype(jnp.float32)
        for h in range(heads):
            key_w[h * key_part : (h + 1) * key_part, :] = (
                wide[pl.ds(h, latent, stride=heads), :].T.astype(BF16)
            )
        wide[...] = value_stage[...].astype(jnp.float32)
        for h in range(heads):
            value_w[:, h * size : (h + 1) * size] = (
                wide[pl.ds(h, latent, stride=heads), :].astype(BF16)
            )

    @pl.when(below & above)
    def _():
        for k in range(slabs):
            remote(
                lat.at[first, :, pl.ds(k * LANES, LANES)],
                mid.at[1 % ways, 0, 0, pl.ds(k * blk, blk)],
                mid_got.at[1 % ways, 0, 0], {"group": g - 1},
            ).start()

    for k in range(slabs):
        lat_load(first, k, 1).wait()

    @pl.loop(1, seqs)
    def _(b):
        for k in range(slabs):
            lat_load(partner(first, b, seqs), k, 0).wait()

    rot_load.wait()

    @pl.loop(0, seqs)
    def _(s):
        block = rot_stage[s].astype(jnp.float32)
        both = jnp.concatenate([block[:half], block[half:]], axis=1)
        stage[s, pl.ds(tail, half), :] = both.astype(BF16)

    @pl.when(below & above)
    def _():
        out(1, 1, first, rot_part, g - 1).start()
        rest(1, g - 1)
        pl.when(jnp.logical_not(inner(1, 1)))(lambda: own_along(g - 1).start())
        pl.semaphore_wait(ready.at[0], 1)
        out(0, 1, first, whole, g + 1).start()
        rest(0, g + 1)
        pl.when(jnp.logical_not(inner(0, 1)))(lambda: own_along(g + 1).start())

    @pl.when(below & (g == planes - 1))
    def _():
        own_along(g - 1).start()

    @pl.when(above & (g == 0))
    def _():
        pl.semaphore_wait(ready.at[0], 1)
        own_along(g + 1).start()

    @pl.loop(c, seqs)
    def _(t):
        @pl.when(join(c, t, seqs) == t)
        def _():
            @pl.when(t > c)
            def _():
                pl.semaphore_wait(ready.at[1 + t], 1)

            @pl.loop(1, seqs)
            def _(i):
                s = partner(c, i, seqs)

                @pl.when(join(c, s, seqs) == t)
                def _():
                    own_side(s).start()

    raw[c, g] = stage[c]
    prepare()

    low = 2 * g < planes

    def near_first(go):
        pl.when(low)(lambda: go(1))
        go(0)
        pl.when(jnp.logical_not(low))(lambda: go(1))

    def arrived(p, q):
        relay(p, q, g).wait_recv()

    def plane(way, far):
        return g - far if way == 0 else g + far

    def exists(way, far):
        return g >= far if way == 0 else g + far < planes

    def onward(way):
        return above if way == 0 else below

    def towards(way):
        return g + 1 if way == 0 else g - 1

    def along(far):
        def go(way):
            @pl.when(exists(way, far))
            def _():
                arrived(plane(way, far), c)

                @pl.when(onward(way))
                def _():
                    relay(plane(way, far), c, towards(way)).start()

        near_first(go)

    def sized(way, go):
        if way == 0 or not give:
            go(whole)
        else:
            pl.when(c > 0)(lambda: go(whole))
            pl.when(c == 0)(lambda: go(kept))

    def pass_mid(far, i):
        def go(way):
            s = partner(c, i, seqs)

            @pl.when(inner(way, far))
            def _():
                if far == 1:
                    out(way, i, c, whole, g).wait_recv()
                    scatter(way, 0, i, whole, plane(way, far), s).start()

                    @pl.when(onward(way))
                    def _():
                        sized(way, lambda part: forward(way, i, part, towards(way)).start())
                else:
                    def onto(part):
                        forward(way, i, part, g).wait_recv()
                        scatter(way, 1, i, part, plane(way, far), s).start()

                    sized(way, onto)

        near_first(go)

    def take(far, i, chain=None):
        def go(way):
            wanted = exists(way, far)
            if chain is not None:
                wanted = wanted & (inner(way, far) != chain)

            @pl.when(wanted)
            def _():
                q = source(c, i, seqs)
                arrived(plane(way, far), q)

                @pl.when(onward(way) & ((far > 1) | jnp.logical_not(inner(way, 1))))
                def _():
                    relay(plane(way, far), q, towards(way)).start()

                if way == 1 and give:
                    @pl.when(below & inner(1, 1) & (far == 1) & (q == 0))
                    def _():
                        relay_given(plane(way, far), q, g - 1).start()

        near_first(go)

    end_q, end_u = pending(c, g, seqs, planes, units)

    def settle(q, low_far, high_far):
        @pl.loop(0, units)
        def _(u):
            far = jnp.maximum(g - u * per_unit, (u + 1) * per_unit - 1 - g)
            far = jnp.maximum(far, 1)
            wanted = (far >= low_far) & (far <= high_far)

            @pl.when(wanted & ((q != end_q) | (u != end_u)))
            def _():
                begin = u * per_unit
                start = pl.multiple_of((q * planes + begin) * blk, LANES)

                def block(row, count):
                    return raw[q, pl.ds(begin, per_unit), row : row + count, :]

                def put_keys(h, wide_keys, turned):
                    keys[h, :key_part, pl.ds(start, LANES)] = wide_keys
                    keys[h, key_part:, pl.ds(start, LANES)] = turned

                def put_values(rows):
                    at = pl.multiple_of(start * heads, LANES * heads)
                    values[pl.ds(at, LANES * heads), :] = rows

                expand(
                    block, slabs, blk, per_unit, heads, rotary, gain, key_w, value_w, mixed,
                    put_keys, put_values,
                )

    def own(i):
        q = source(c, i, seqs)
        arrived(g, q)

        @pl.when(above & (g == 0))
        def _():
            relay(g, q, g + 1).start()

        @pl.when(below & (g == planes - 1))
        def _():
            relay(g, q, g - 1).start()

    @pl.loop(1, seqs)
    def _(i):
        pl.when(g == planes - 1)(lambda: own(i))
        pl.when((g < planes - 1) | (g == 0))(lambda: pass_mid(1, i))
        pl.when((g == 0) & above)(lambda: own(i))

    @pl.loop(1, seqs)
    def _(i):
        pl.when((g == planes - 1) & below)(lambda: pass_mid(1, i))

    pl.when(inner(1, 1) & below)(lambda: own_along(g - 1).start())
    pl.when(inner(0, 1) & above)(lambda: own_along(g + 1).start())
    pl.when(jnp.logical_not(edge))(lambda: along(1))

    @pl.when(jnp.logical_not(edge))
    def _():
        settle(c, 1, 1)

        @pl.loop(1, seqs)
        def _(i):
            take(1, i, True)

    @pl.loop(1, seqs + 1)
    def _(i):
        @pl.when(i < seqs)
        def _():
            pass_mid(2, i)
            pl.when(jnp.logical_not(edge))(lambda: own(i))
            pl.when(edge)(lambda: take(1, i))
            pl.when(jnp.logical_not(edge))(lambda: take(1, i, False))

        @pl.when((i == seqs) & edge)
        def _():
            along(1)

        @pl.when((i < seqs) | edge)
        def _():
            settle(jnp.where(i == seqs, c, source(c, i, seqs)), 1, 1)

    along(2)

    def drain():
        ups, downs = jnp.minimum(planes - 1 - g, 1), jnp.minimum(g, 1)
        total = seqs * (ups + downs + g * ups + (planes - 1 - g) * downs)
        spread = sum(jnp.where(inner(way, far), 1, 0) for way in (0, 1) for far in (1, 2))
        total = total + (seqs - 1) * (1 + spread)
        near, next_near = jnp.where(inner(1, 1) & below, 1, 0), jnp.where(inner(1, 2), 1, 0)
        parts = jnp.where(c == 0, (seqs - 1) * (near + next_near), 0)
        if not give:
            parts = 0 * parts

        @pl.loop(0, total - parts)
        def _(_):
            own_along(g).wait_send()

        @pl.loop(0, parts)
        def _(_):
            forward(1, 1, kept, g).wait_send()

        if give:
            @pl.when((c > 0) & (near > 0))
            def _():
                relay_given(g, c, g).wait_send()

    pl.when(edge)(drain)

    def origin(i):
        return jnp.where(i == 0, c, source(c, jnp.maximum(i, 0), seqs))

    @pl.loop(2, max(planes, 3))
    def _(far):
        turn = gate & (far == planes - 2)

        @pl.loop(0, seqs + 1)
        def _(i):
            @pl.when((i == 0) & (far > 2))
            def _():
                along(far)

            @pl.when(turn & (ens == 1) & (i == max(seqs - HELD, 1)))
            def _():
                pl.semaphore_wait(ready.at[1], 1)

            at = jnp.where(edge, i, i - 1)
            late = turn & (ens == 1) & (i == seqs - 1) & (c == 0)
            pl.when(late)(lambda: settle(origin(at), far, far))

            @pl.when((i > 0) & (i < seqs))
            def _():
                take(far, i)

            done = turn & (ens == 0) & (i == seqs - 1)

            def release():
                pl.semaphore_signal(ready.at[1], inc=1, device_id={"ens": 1}, device_id_type=MESH)

            pl.when(done & (c > 0))(release)

            @pl.when((at >= 0) & (at < seqs) & jnp.logical_not(late))
            def _():
                settle(origin(at), far, far)

            pl.when(done & (c == 0))(release)

    last[...] = raw[end_q, pl.ds(end_u * per_unit, per_unit)]

    pl.when(jnp.logical_not(edge))(drain)


def store(
    seqs, planes, heads, rotary, blk,
    keys, values, last, key_w, value_w, gain,
    keys_out, values_out,
    end_keys, end_values, mixed, sems,
):
    c, g = lax.axis_index("ctx"), lax.axis_index("group")
    slabs = gain.shape[1] // LANES
    per_unit = LANES // blk
    units = planes // per_unit
    key_part = key_w.shape[0] // heads
    blocks = seqs * units
    end_q, end_u = pending(c, g, seqs, planes, units)
    end = end_q * units + end_u

    def columns(b):
        return pl.ds(pl.multiple_of(b * LANES, LANES), LANES)

    def rows(b):
        return pl.ds(pl.multiple_of(b * LANES * heads, LANES * heads), LANES * heads)

    @pl.loop(1, blocks)
    def _(j):
        b = lax.rem(end + j, blocks)
        pltpu.make_async_copy(
            keys.at[:, :, columns(b)], keys_out.at[:, :, columns(b)], sems.at[0]
        ).start()
        pltpu.make_async_copy(values.at[rows(b)], values_out.at[rows(b)], sems.at[1]).start()

    def block(row, count):
        return last[:, row : row + count, :]

    def put_keys(h, wide_keys, turned):
        end_keys[h, :key_part, :] = wide_keys
        end_keys[h, key_part:, :] = turned

    def put_values(part):
        end_values[...] = part

    expand(
        block, slabs, blk, per_unit, heads, rotary, gain, key_w, value_w, mixed,
        put_keys, put_values,
    )
    pltpu.make_async_copy(end_keys, keys_out.at[:, :, columns(end)], sems.at[0]).start()
    pltpu.make_async_copy(end_values, values_out.at[rows(end)], sems.at[1]).start()
    pltpu.make_async_copy(keys, keys_out, sems.at[0]).wait()
    pltpu.make_async_copy(values, values_out, sems.at[1]).wait()


def per_device(latents, rotary_rows, latent_gain, key_up, value_up):
    seqs, planes = lax.axis_size("ctx"), lax.axis_size("group")
    _, blk, latent = latents.shape
    rotary = rotary_rows.shape[2]
    heads, key_part = key_up.shape[1:]
    size = value_up.shape[2]
    length = seqs * planes * blk
    per_unit = LANES // blk
    ways = 1 if planes <= 4 else 2
    packed = (blk * (latent + rotary) // LANES, LANES)
    dma = pltpu.SemaphoreType.DMA
    in_hbm = functools.partial(pltpu.with_memory_space_constraint, memory_space=pltpu.HBM)
    outer = pl.BlockSpec(memory_space=pltpu.HBM)
    inside = pl.BlockSpec(memory_space=pltpu.VMEM)
    held = pl.pallas_call(
        functools.partial(kernel, seqs, planes, heads, rotary),
        out_shape=(
            pltpu.VMEM((heads, key_part + rotary, length), BF16),
            pltpu.VMEM((length * heads, size), BF16),
            pltpu.VMEM((per_unit, *packed), BF16),
            pltpu.VMEM((heads * key_part, latent), BF16),
            pltpu.VMEM((latent, heads * size), BF16),
            pltpu.VMEM((1, latent), jnp.float32),
        ),
        in_specs=[outer] * 5,
        out_specs=(inside,) * 6,
        scratch_shapes=[
            pltpu.VMEM((seqs, *packed), BF16),
            pltpu.VMEM((seqs, planes, *packed), BF16),
            pltpu.VMEM((ways, 2, seqs - 1, *packed), BF16),
            pltpu.VMEM((seqs, blk, rotary), BF16),
            pltpu.VMEM((latent * heads, key_part), BF16),
            pltpu.VMEM((latent * heads, size), BF16),
            pltpu.VMEM((latent * heads, size), jnp.float32),
            pltpu.VMEM((LANES * heads, size), jnp.float32),
            dma((3,)),
            dma((planes, seqs)),
            dma((ways, 2, seqs - 1)),
            dma,
            pltpu.SemaphoreType.REGULAR((1 + seqs,)),
        ],
        compiler_params=pltpu.CompilerParams(
            collective_id=0, has_side_effects=True, vmem_limit_bytes=32 * 1024 * 1024
        ),
    )(
        in_hbm(latents),
        in_hbm(rotary_rows),
        in_hbm(latent_gain.reshape(1, latent)),
        in_hbm(key_up.reshape(latent * heads, key_part)),
        in_hbm(value_up.reshape(latent * heads, size)),
    )
    keys, values = pl.pallas_call(
        functools.partial(store, seqs, planes, heads, rotary, blk),
        out_shape=(
            jax.ShapeDtypeStruct((heads, key_part + rotary, length), BF16),
            jax.ShapeDtypeStruct((length * heads, size), BF16),
        ),
        in_specs=[inside] * 6,
        out_specs=(outer, outer),
        scratch_shapes=[
            pltpu.VMEM((heads, key_part + rotary, LANES), BF16),
            pltpu.VMEM((LANES * heads, size), BF16),
            pltpu.VMEM((LANES * heads, size), jnp.float32),
            dma((2,)),
        ],
        compiler_params=pltpu.CompilerParams(vmem_limit_bytes=16 * 1024 * 1024),
    )(*held)
    return keys[None], values.reshape(1, length, heads, size)


def solution(mesh):
    in_specs = (
        P("ens", ("ctx", "group"), None),
        P("ens", ("ctx", "group"), None),
        P(),
        P("ens", "group", None),
        P("ens", "group", None),
    )
    out_specs = (P(("ens", "ctx"), "group", None, None), P(("ens", "ctx"), None, "group", None))
    return jax.shard_map(
        per_device, mesh=mesh, in_specs=in_specs, out_specs=out_specs, check_vma=False
    )
```

```python
import functools

import jax
import jax.numpy as jnp
from jax import lax
from jax.experimental import pallas as pl
from jax.experimental.pallas import tpu as pltpu
from jax.sharding import PartitionSpec as P

MESH = pl.DeviceIdType.MESH
LANES = 128
BF16 = jnp.bfloat16
GIVEN = 3, 18
HELD = 1


def xor(me, step, count):
    total, bit = 0, 1
    while bit < count:
        total = total + bit * lax.rem(me // bit + step // bit, 2)
        bit *= 2
    return total


def partner(me, step, count):
    return lax.rem(me + step, count) if count & (count - 1) else xor(me, step, count)


def source(me, step, count):
    return lax.rem(me + count - step, count) if count & (count - 1) else xor(me, step, count)


def join(a, b, count):
    if count & (count - 1):
        return jnp.maximum(a, b)
    total, bit = 0, 1
    while bit < count:
        total = total + bit * jnp.maximum(lax.rem(a // bit, 2), lax.rem(b // bit, 2))
        bit *= 2
    return total


def lower(c, count):
    if count & (count - 1):
        return c
    total, bit = 1, 1
    while bit < count:
        total = total * (1 + lax.rem(c // bit, 2))
        bit *= 2
    return total - 1


def pending(c, g, seqs, planes, units):
    q = source(c, seqs - 1, seqs) if seqs > 1 else c
    return q, jnp.where(2 * g < planes, units - 1, 0)


def expand(block, slabs, blk, per_unit, heads, rotary, gain, key_w, value_w, mixed, put_keys, put_values):
    key_part = key_w.shape[0] // heads
    size = value_w.shape[1] // heads
    x = jnp.concatenate(
        [block(k * blk, blk).astype(jnp.float32).reshape(LANES, LANES) for k in range(slabs)],
        axis=1,
    )
    mean = jnp.mean(x * x, axis=-1, keepdims=True)
    rows = (x * lax.rsqrt(mean + 1e-06) * gain[...]).astype(BF16)
    wide_keys = lax.dot_general(
        key_w[...], rows, (((1,), (1,)), ((), ())), preferred_element_type=jnp.float32
    ).astype(BF16)
    tails = block(slabs * blk, blk * rotary // LANES).astype(jnp.float32)
    pieces = []
    for j in range(per_unit):
        pieces += [tails[j][:, :rotary], pltpu.roll(tails[j], rotary, 1)[:, :rotary]]
    turned = jnp.concatenate(pieces, axis=0).T.astype(BF16)
    for h in range(heads):
        put_keys(h, wide_keys[h * key_part : (h + 1) * key_part], turned)
    wide_values = jnp.dot(rows, value_w[...], preferred_element_type=jnp.float32)
    for h in range(heads):
        mixed[pl.ds(h, LANES, stride=heads), :] = wide_values[:, h * size : (h + 1) * size]
    put_values(mixed[...].astype(BF16))


def kernel(
    seqs, planes, heads, rotary,
    lat, rot, gain_in, key_up, value_up,
    keys, values, last, key_w, value_w, gain,
    stage, raw, mid, rot_stage, key_stage, value_stage, wide, mixed,
    load_sem, got, mid_got, sent, ready,
):
    ens, c, g = lax.axis_index("ens"), lax.axis_index("ctx"), lax.axis_index("group")
    blk, latent = lat.shape[1:]
    slabs = latent // LANES
    tail = slabs * blk
    half = blk // 2
    give = stage.shape[1] // 16 * GIVEN[0] // GIVEN[1] * 16
    keep = stage.shape[1] - give
    kept, given = pl.ds(0, keep), pl.ds(keep, give)
    ways = mid.shape[0]
    per_unit = LANES // blk
    units = planes // per_unit
    key_part = key_w.shape[0] // heads
    size = value_w.shape[1] // heads
    first = partner(c, 1, seqs)

    def lat_load(s, k, sem):
        return pltpu.make_async_copy(
            lat.at[s, :, pl.ds(k * LANES, LANES)],
            stage.at[s, pl.ds(k * blk, blk), :],
            load_sem.at[sem],
        )

    rot_load = pltpu.make_async_copy(rot, rot_stage, load_sem.at[0])
    for k in range(slabs):
        lat_load(first, k, 1).start()
    rot_load.start()

    @pl.loop(1, seqs)
    def _(b):
        for k in range(slabs):
            lat_load(partner(first, b, seqs), k, 0).start()

    loads = [
        pltpu.make_async_copy(key_up, key_stage, load_sem.at[2]),
        pltpu.make_async_copy(value_up, value_stage, load_sem.at[2]),
        pltpu.make_async_copy(gain_in, gain, load_sem.at[2]),
    ]
    for load in loads:
        load.start()

    barrier = pltpu.get_barrier_semaphore()
    above, below = g < planes - 1, g > 0
    edge = (g == 0) | (g == planes - 1)
    gate = (g == 1) | (g == planes - 2) if planes > 3 else g < 0

    def inner(way, far):
        return g > far if way == 0 else g + far < planes - 1

    @pl.when(above)
    def _():
        pl.semaphore_signal(barrier, inc=1, device_id={"group": g + 1}, device_id_type=MESH)

    @pl.when(gate & (ens == 1))
    def _():
        pl.semaphore_signal(barrier, inc=1, device_id={"ens": 0}, device_id_type=MESH)

    @pl.loop(c + 1, seqs)
    def _(s):
        @pl.when(join(c, s, seqs) == s)
        def _():
            pl.semaphore_signal(barrier, inc=1, device_id={"ctx": s}, device_id_type=MESH)

    def remote(src, dst, in_sem, to):
        return pltpu.make_async_remote_copy(
            src_ref=src, dst_ref=dst, send_sem=sent, recv_sem=in_sem,
            device_id=to, device_id_type=MESH,
        )

    def out(way, i, s, part, to):
        return remote(
            stage.at[s, part], mid.at[way % ways, 0, i - 1, part], mid_got.at[way % ways, 0, i - 1], {"group": to}
        )

    def own_along(to):
        return remote(stage.at[c], raw.at[c, g], got.at[g, c], {"group": to})

    def own_side(s):
        return remote(stage.at[s], raw.at[c, g], got.at[g, c], {"ctx": s})

    def forward(way, i, part, to):
        return remote(
            mid.at[way % ways, 0, i - 1, part], mid.at[way % ways, 1, i - 1, part],
            mid_got.at[way % ways, 1, i - 1], {"group": to},
        )

    def scatter(way, far, i, part, p, s):
        return remote(mid.at[way % ways, far, i - 1, part], raw.at[c, p, part], got.at[p, c], {"ctx": s})

    def relay(p, q, to):
        return remote(raw.at[q, p], raw.at[q, p], got.at[p, q], {"group": to})

    def relay_given(p, q, to):
        return remote(raw.at[q, p, given], raw.at[q, p, given], got.at[p, q], {"group": to})

    whole = pl.ds(0, stage.shape[1])
    wide_part, rot_part = pl.ds(0, tail), pl.ds(tail, half)

    def rest(way, to):
        @pl.loop(2, seqs)
        def _(i):
            out(way, i, partner(c, i, seqs), whole, to).start()

    early = lower(c, seqs) + jnp.minimum(g, 1) + jnp.where(gate & (ens == 0), 1, 0)

    @pl.when(early > 0)
    def _():
        pl.semaphore_wait(barrier, early)

    @pl.when(below)
    def _():
        pl.semaphore_signal(ready.at[0], inc=1, device_id={"group": g - 1}, device_id_type=MESH)

    @pl.loop(0, c)
    def _(s):
        @pl.when(join(c, s, seqs) == c)
        def _():
            pl.semaphore_signal(ready.at[1 + c], inc=1, device_id={"ctx": s}, device_id_type=MESH)

    def prepare():
        for load in loads:
            load.wait()
        wide[...] = key_stage[...].astype(jnp.float32)
        for h in range(heads):
            key_w[h * key_part : (h + 1) * key_part, :] = (
                wide[pl.ds(h, latent, stride=heads), :].T.astype(BF16)
            )
        wide[...] = value_stage[...].astype(jnp.float32)
        for h in range(heads):
            value_w[:, h * size : (h + 1) * size] = (
                wide[pl.ds(h, latent, stride=heads), :].astype(BF16)
            )

    @pl.when(below & above)
    def _():
        for k in range(slabs):
            remote(
                lat.at[first, :, pl.ds(k * LANES, LANES)],
                mid.at[1 % ways, 0, 0, pl.ds(k * blk, blk)],
                mid_got.at[1 % ways, 0, 0], {"group": g - 1},
            ).start()

    for k in range(slabs):
        lat_load(first, k, 1).wait()

    @pl.loop(1, seqs)
    def _(b):
        for k in range(slabs):
            lat_load(partner(first, b, seqs), k, 0).wait()

    rot_load.wait()

    @pl.loop(0, seqs)
    def _(b):
        s = partner(first, b, seqs)
        block = rot_stage[s].astype(jnp.float32)
        both = jnp.concatenate([block[:half], block[half:]], axis=1)
        stage[s, pl.ds(tail, half), :] = both.astype(BF16)

    @pl.when(below & above)
    def _():
        out(1, 1, first, rot_part, g - 1).start()
        rest(1, g - 1)
        pl.when(jnp.logical_not(inner(1, 1)))(lambda: own_along(g - 1).start())
        pl.semaphore_wait(ready.at[0], 1)
        out(0, 1, first, whole, g + 1).start()
        rest(0, g + 1)
        pl.when(jnp.logical_not(inner(0, 1)))(lambda: own_along(g + 1).start())

    @pl.when(below & (g == planes - 1))
    def _():
        own_along(g - 1).start()

    @pl.when(above & (g == 0))
    def _():
        pl.semaphore_wait(ready.at[0], 1)
        own_along(g + 1).start()

    @pl.loop(c, seqs)
    def _(t):
        @pl.when(join(c, t, seqs) == t)
        def _():
            @pl.when(t > c)
            def _():
                pl.semaphore_wait(ready.at[1 + t], 1)

            @pl.loop(1, seqs)
            def _(i):
                s = partner(c, i, seqs)

                @pl.when(join(c, s, seqs) == t)
                def _():
                    own_side(s).start()

    raw[c, g] = stage[c]
    prepare()

    low = 2 * g < planes

    def near_first(go):
        pl.when(low)(lambda: go(1))
        go(0)
        pl.when(jnp.logical_not(low))(lambda: go(1))

    def arrived(p, q):
        relay(p, q, g).wait_recv()

    def plane(way, far):
        return g - far if way == 0 else g + far

    def exists(way, far):
        return g >= far if way == 0 else g + far < planes

    def onward(way):
        return above if way == 0 else below

    def towards(way):
        return g + 1 if way == 0 else g - 1

    def along(far):
        def go(way):
            @pl.when(exists(way, far))
            def _():
                arrived(plane(way, far), c)

                @pl.when(onward(way))
                def _():
                    relay(plane(way, far), c, towards(way)).start()

        near_first(go)

    def sized(way, go):
        if way == 0 or not give:
            go(whole)
        else:
            pl.when(c > 0)(lambda: go(whole))
            pl.when(c == 0)(lambda: go(kept))

    def pass_mid(far, i):
        def go(way):
            s = partner(c, i, seqs)

            @pl.when(inner(way, far))
            def _():
                if far == 1:
                    out(way, i, c, whole, g).wait_recv()
                    scatter(way, 0, i, whole, plane(way, far), s).start()

                    @pl.when(onward(way))
                    def _():
                        sized(way, lambda part: forward(way, i, part, towards(way)).start())
                else:
                    def onto(part):
                        forward(way, i, part, g).wait_recv()
                        scatter(way, 1, i, part, plane(way, far), s).start()

                    sized(way, onto)

        near_first(go)

    def take(far, i, chain=None):
        def go(way):
            wanted = exists(way, far)
            if chain is not None:
                wanted = wanted & (inner(way, far) != chain)

            @pl.when(wanted)
            def _():
                q = source(c, i, seqs)
                arrived(plane(way, far), q)

                @pl.when(onward(way) & ((far > 1) | jnp.logical_not(inner(way, 1))))
                def _():
                    relay(plane(way, far), q, towards(way)).start()

                if way == 1 and give:
                    @pl.when(below & inner(1, 1) & (far == 1) & (q == 0))
                    def _():
                        relay_given(plane(way, far), q, g - 1).start()

        near_first(go)

    end_q, end_u = pending(c, g, seqs, planes, units)

    def settle(q, low_far, high_far):
        @pl.loop(0, units)
        def _(u):
            far = jnp.maximum(g - u * per_unit, (u + 1) * per_unit - 1 - g)
            far = jnp.maximum(far, 1)
            wanted = (far >= low_far) & (far <= high_far)

            @pl.when(wanted & ((q != end_q) | (u != end_u)))
            def _():
                begin = u * per_unit
                start = pl.multiple_of((q * planes + begin) * blk, LANES)

                def block(row, count):
                    return raw[q, pl.ds(begin, per_unit), row : row + count, :]

                def put_keys(h, wide_keys, turned):
                    keys[h, :key_part, pl.ds(start, LANES)] = wide_keys
                    keys[h, key_part:, pl.ds(start, LANES)] = turned

                def put_values(rows):
                    at = pl.multiple_of(start * heads, LANES * heads)
                    values[pl.ds(at, LANES * heads), :] = rows

                expand(
                    block, slabs, blk, per_unit, heads, rotary, gain, key_w, value_w, mixed,
                    put_keys, put_values,
                )

    def own(i):
        q = source(c, i, seqs)
        arrived(g, q)

        @pl.when(above & (g == 0))
        def _():
            relay(g, q, g + 1).start()

        @pl.when(below & (g == planes - 1))
        def _():
            relay(g, q, g - 1).start()

    @pl.loop(1, seqs)
    def _(i):
        pl.when(g == planes - 1)(lambda: own(i))
        pl.when((g < planes - 1) | (g == 0))(lambda: pass_mid(1, i))
        pl.when((g == 0) & above)(lambda: own(i))

    @pl.loop(1, seqs)
    def _(i):
        pl.when((g == planes - 1) & below)(lambda: pass_mid(1, i))

    pl.when(inner(1, 1) & below)(lambda: own_along(g - 1).start())
    pl.when(inner(0, 1) & above)(lambda: own_along(g + 1).start())
    pl.when(jnp.logical_not(edge))(lambda: along(1))

    @pl.when(jnp.logical_not(edge))
    def _():
        settle(c, 1, 1)

        @pl.loop(1, seqs)
        def _(i):
            take(1, i, True)

    @pl.loop(1, seqs + 1)
    def _(i):
        @pl.when(i < seqs)
        def _():
            pass_mid(2, i)
            pl.when(jnp.logical_not(edge))(lambda: own(i))
            pl.when(edge)(lambda: take(1, i))
            pl.when(jnp.logical_not(edge))(lambda: take(1, i, False))

        @pl.when((i == seqs) & edge)
        def _():
            along(1)

        @pl.when((i < seqs) | edge)
        def _():
            settle(jnp.where(i == seqs, c, source(c, i, seqs)), 1, 1)

    along(2)

    def drain():
        ups, downs = jnp.minimum(planes - 1 - g, 1), jnp.minimum(g, 1)
        total = seqs * (ups + downs + g * ups + (planes - 1 - g) * downs)
        spread = sum(jnp.where(inner(way, far), 1, 0) for way in (0, 1) for far in (1, 2))
        total = total + (seqs - 1) * (1 + spread)
        near, next_near = jnp.where(inner(1, 1) & below, 1, 0), jnp.where(inner(1, 2), 1, 0)
        parts = jnp.where(c == 0, (seqs - 1) * (near + next_near), 0)
        if not give:
            parts = 0 * parts

        @pl.loop(0, total - parts)
        def _(_):
            own_along(g).wait_send()

        @pl.loop(0, parts)
        def _(_):
            forward(1, 1, kept, g).wait_send()

        if give:
            @pl.when((c > 0) & (near > 0))
            def _():
                relay_given(g, c, g).wait_send()

    pl.when(edge)(drain)

    def origin(i):
        return jnp.where(i == 0, c, source(c, jnp.maximum(i, 0), seqs))

    @pl.loop(2, max(planes, 3))
    def _(far):
        turn = gate & (far == planes - 2)

        @pl.loop(0, seqs + 1)
        def _(i):
            @pl.when((i == 0) & (far > 2))
            def _():
                along(far)

            @pl.when(turn & (ens == 1) & (i == max(seqs - HELD, 1)))
            def _():
                pl.semaphore_wait(ready.at[1], 1)

            at = jnp.where(edge, i, i - 1)
            late = turn & (ens == 1) & (i == seqs - 1) & (c == 0)
            pl.when(late)(lambda: settle(origin(at), far, far))

            @pl.when((i > 0) & (i < seqs))
            def _():
                take(far, i)

            done = turn & (ens == 0) & (i == seqs - 1)

            def release():
                pl.semaphore_signal(ready.at[1], inc=1, device_id={"ens": 1}, device_id_type=MESH)

            pl.when(done & (c > 0))(release)

            @pl.when((at >= 0) & (at < seqs) & jnp.logical_not(late))
            def _():
                settle(origin(at), far, far)

            pl.when(done & (c == 0))(release)

    last[...] = raw[end_q, pl.ds(end_u * per_unit, per_unit)]

    pl.when(jnp.logical_not(edge))(drain)


def store(
    seqs, planes, heads, rotary, blk,
    keys, values, last, key_w, value_w, gain,
    keys_out, values_out,
    end_keys, end_values, mixed, sems,
):
    c, g = lax.axis_index("ctx"), lax.axis_index("group")
    slabs = gain.shape[1] // LANES
    per_unit = LANES // blk
    units = planes // per_unit
    key_part = key_w.shape[0] // heads
    blocks = seqs * units
    end_q, end_u = pending(c, g, seqs, planes, units)
    end = end_q * units + end_u

    def columns(b):
        return pl.ds(pl.multiple_of(b * LANES, LANES), LANES)

    def rows(b):
        return pl.ds(pl.multiple_of(b * LANES * heads, LANES * heads), LANES * heads)

    @pl.loop(1, blocks)
    def _(j):
        b = lax.rem(end + j, blocks)
        pltpu.make_async_copy(
            keys.at[:, :, columns(b)], keys_out.at[:, :, columns(b)], sems.at[0]
        ).start()
        pltpu.make_async_copy(values.at[rows(b)], values_out.at[rows(b)], sems.at[1]).start()

    def block(row, count):
        return last[:, row : row + count, :]

    def put_keys(h, wide_keys, turned):
        end_keys[h, :key_part, :] = wide_keys
        end_keys[h, key_part:, :] = turned

    def put_values(part):
        end_values[...] = part

    expand(
        block, slabs, blk, per_unit, heads, rotary, gain, key_w, value_w, mixed,
        put_keys, put_values,
    )
    pltpu.make_async_copy(end_keys, keys_out.at[:, :, columns(end)], sems.at[0]).start()
    pltpu.make_async_copy(end_values, values_out.at[rows(end)], sems.at[1]).start()
    pltpu.make_async_copy(keys, keys_out, sems.at[0]).wait()
    pltpu.make_async_copy(values, values_out, sems.at[1]).wait()


def per_device(latents, rotary_rows, latent_gain, key_up, value_up):
    seqs, planes = lax.axis_size("ctx"), lax.axis_size("group")
    _, blk, latent = latents.shape
    rotary = rotary_rows.shape[2]
    heads, key_part = key_up.shape[1:]
    size = value_up.shape[2]
    length = seqs * planes * blk
    per_unit = LANES // blk
    ways = 1 if planes <= 4 else 2
    packed = (blk * (latent + rotary) // LANES, LANES)
    dma = pltpu.SemaphoreType.DMA
    in_hbm = functools.partial(pltpu.with_memory_space_constraint, memory_space=pltpu.HBM)
    outer = pl.BlockSpec(memory_space=pltpu.HBM)
    inside = pl.BlockSpec(memory_space=pltpu.VMEM)
    held = pl.pallas_call(
        functools.partial(kernel, seqs, planes, heads, rotary),
        out_shape=(
            pltpu.VMEM((heads, key_part + rotary, length), BF16),
            pltpu.VMEM((length * heads, size), BF16),
            pltpu.VMEM((per_unit, *packed), BF16),
            pltpu.VMEM((heads * key_part, latent), BF16),
            pltpu.VMEM((latent, heads * size), BF16),
            pltpu.VMEM((1, latent), jnp.float32),
        ),
        in_specs=[outer] * 5,
        out_specs=(inside,) * 6,
        scratch_shapes=[
            pltpu.VMEM((seqs, *packed), BF16),
            pltpu.VMEM((seqs, planes, *packed), BF16),
            pltpu.VMEM((ways, 2, seqs - 1, *packed), BF16),
            pltpu.VMEM((seqs, blk, rotary), BF16),
            pltpu.VMEM((latent * heads, key_part), BF16),
            pltpu.VMEM((latent * heads, size), BF16),
            pltpu.VMEM((latent * heads, size), jnp.float32),
            pltpu.VMEM((LANES * heads, size), jnp.float32),
            dma((3,)),
            dma((planes, seqs)),
            dma((ways, 2, seqs - 1)),
            dma,
            pltpu.SemaphoreType.REGULAR((1 + seqs,)),
        ],
        compiler_params=pltpu.CompilerParams(
            collective_id=0, has_side_effects=True, vmem_limit_bytes=32 * 1024 * 1024
        ),
    )(
        in_hbm(latents),
        in_hbm(rotary_rows),
        in_hbm(latent_gain.reshape(1, latent)),
        in_hbm(key_up.reshape(latent * heads, key_part)),
        in_hbm(value_up.reshape(latent * heads, size)),
    )
    keys, values = pl.pallas_call(
        functools.partial(store, seqs, planes, heads, rotary, blk),
        out_shape=(
            jax.ShapeDtypeStruct((heads, key_part + rotary, length), BF16),
            jax.ShapeDtypeStruct((length * heads, size), BF16),
        ),
        in_specs=[inside] * 6,
        out_specs=(outer, outer),
        scratch_shapes=[
            pltpu.VMEM((heads, key_part + rotary, LANES), BF16),
            pltpu.VMEM((LANES * heads, size), BF16),
            pltpu.VMEM((LANES * heads, size), jnp.float32),
            dma((2,)),
        ],
        compiler_params=pltpu.CompilerParams(vmem_limit_bytes=16 * 1024 * 1024),
    )(*held)
    return keys[None], values.reshape(1, length, heads, size)


def solution(mesh):
    in_specs = (
        P("ens", ("ctx", "group"), None),
        P("ens", ("ctx", "group"), None),
        P(),
        P("ens", "group", None),
        P("ens", "group", None),
    )
    out_specs = (P(("ens", "ctx"), "group", None, None), P(("ens", "ctx"), None, "group", None))
    return jax.shard_map(
        per_device, mesh=mesh, in_specs=in_specs, out_specs=out_specs, check_vma=False
    )
```

```python
import functools

import jax
import jax.numpy as jnp
from jax import lax
from jax.experimental import pallas as pl
from jax.experimental.pallas import tpu as pltpu
from jax.sharding import PartitionSpec as P

MESH = pl.DeviceIdType.MESH
LANES = 128
BF16 = jnp.bfloat16
GIVEN = 2, 18
HELD = 1


def xor(me, step, count):
    total, bit = 0, 1
    while bit < count:
        total = total + bit * lax.rem(me // bit + step // bit, 2)
        bit *= 2
    return total


def partner(me, step, count):
    return lax.rem(me + step, count) if count & (count - 1) else xor(me, step, count)


def source(me, step, count):
    return lax.rem(me + count - step, count) if count & (count - 1) else xor(me, step, count)


def join(a, b, count):
    if count & (count - 1):
        return jnp.maximum(a, b)
    total, bit = 0, 1
    while bit < count:
        total = total + bit * jnp.maximum(lax.rem(a // bit, 2), lax.rem(b // bit, 2))
        bit *= 2
    return total


def lower(c, count):
    if count & (count - 1):
        return c
    total, bit = 1, 1
    while bit < count:
        total = total * (1 + lax.rem(c // bit, 2))
        bit *= 2
    return total - 1


def pending(c, g, seqs, planes, units):
    q = source(c, seqs - 1, seqs) if seqs > 1 else c
    return q, jnp.where(2 * g < planes, units - 1, 0)


def expand(block, slabs, blk, per_unit, heads, rotary, gain, key_w, value_w, mixed, put_keys, put_values):
    key_part = key_w.shape[0] // heads
    size = value_w.shape[1] // heads
    x = jnp.concatenate(
        [block(k * blk, blk).astype(jnp.float32).reshape(LANES, LANES) for k in range(slabs)],
        axis=1,
    )
    mean = jnp.mean(x * x, axis=-1, keepdims=True)
    rows = (x * lax.rsqrt(mean + 1e-06) * gain[...]).astype(BF16)
    wide_keys = lax.dot_general(
        key_w[...], rows, (((1,), (1,)), ((), ())), preferred_element_type=jnp.float32
    ).astype(BF16)
    tails = block(slabs * blk, blk * rotary // LANES).astype(jnp.float32)
    pieces = []
    for j in range(per_unit):
        pieces += [tails[j][:, :rotary], pltpu.roll(tails[j], rotary, 1)[:, :rotary]]
    turned = jnp.concatenate(pieces, axis=0).T.astype(BF16)
    for h in range(heads):
        put_keys(h, wide_keys[h * key_part : (h + 1) * key_part], turned)
    wide_values = jnp.dot(rows, value_w[...], preferred_element_type=jnp.float32)
    for h in range(heads):
        mixed[pl.ds(h, LANES, stride=heads), :] = wide_values[:, h * size : (h + 1) * size]
    put_values(mixed[...].astype(BF16))


def kernel(
    seqs, planes, heads, rotary,
    lat, rot, gain_in, key_up, value_up,
    keys, values, last, key_w, value_w, gain,
    stage, raw, mid, rot_stage, key_stage, value_stage, wide, mixed,
    load_sem, got, mid_got, sent, ready,
):
    ens, c, g = lax.axis_index("ens"), lax.axis_index("ctx"), lax.axis_index("group")
    blk, latent = lat.shape[1:]
    slabs = latent // LANES
    tail = slabs * blk
    half = blk // 2
    give = stage.shape[1] // 16 * GIVEN[0] // GIVEN[1] * 16
    keep = stage.shape[1] - give
    kept, given = pl.ds(0, keep), pl.ds(keep, give)
    ways = mid.shape[0]
    per_unit = LANES // blk
    units = planes // per_unit
    key_part = key_w.shape[0] // heads
    size = value_w.shape[1] // heads
    first = partner(c, 1, seqs)

    def lat_load(s, k, sem):
        return pltpu.make_async_copy(
            lat.at[s, :, pl.ds(k * LANES, LANES)],
            stage.at[s, pl.ds(k * blk, blk), :],
            load_sem.at[sem],
        )

    rot_load = pltpu.make_async_copy(rot, rot_stage, load_sem.at[0])
    for k in range(slabs):
        lat_load(first, k, 1).start()
    rot_load.start()

    @pl.loop(1, seqs)
    def _(b):
        for k in range(slabs):
            lat_load(partner(first, b, seqs), k, 0).start()

    loads = [
        pltpu.make_async_copy(key_up, key_stage, load_sem.at[2]),
        pltpu.make_async_copy(value_up, value_stage, load_sem.at[2]),
        pltpu.make_async_copy(gain_in, gain, load_sem.at[2]),
    ]
    for load in loads:
        load.start()

    barrier = pltpu.get_barrier_semaphore()
    above, below = g < planes - 1, g > 0
    edge = (g == 0) | (g == planes - 1)
    gate = (g == 1) | (g == planes - 2) if planes > 3 else g < 0

    def inner(way, far):
        return g > far if way == 0 else g + far < planes - 1

    @pl.when(above)
    def _():
        pl.semaphore_signal(barrier, inc=1, device_id={"group": g + 1}, device_id_type=MESH)

    @pl.when(gate & (ens == 1))
    def _():
        pl.semaphore_signal(barrier, inc=1, device_id={"ens": 0}, device_id_type=MESH)

    @pl.loop(c + 1, seqs)
    def _(s):
        @pl.when(join(c, s, seqs) == s)
        def _():
            pl.semaphore_signal(barrier, inc=1, device_id={"ctx": s}, device_id_type=MESH)

    def remote(src, dst, in_sem, to):
        return pltpu.make_async_remote_copy(
            src_ref=src, dst_ref=dst, send_sem=sent, recv_sem=in_sem,
            device_id=to, device_id_type=MESH,
        )

    def out(way, i, s, part, to):
        return remote(
            stage.at[s, part], mid.at[way % ways, 0, i - 1, part], mid_got.at[way % ways, 0, i - 1], {"group": to}
        )

    def own_along(to):
        return remote(stage.at[c], raw.at[c, g], got.at[g, c], {"group": to})

    def own_side(s):
        return remote(stage.at[s], raw.at[c, g], got.at[g, c], {"ctx": s})

    def forward(way, i, part, to):
        return remote(
            mid.at[way % ways, 0, i - 1, part], mid.at[way % ways, 1, i - 1, part],
            mid_got.at[way % ways, 1, i - 1], {"group": to},
        )

    def scatter(way, far, i, part, p, s):
        return remote(mid.at[way % ways, far, i - 1, part], raw.at[c, p, part], got.at[p, c], {"ctx": s})

    def relay(p, q, to):
        return remote(raw.at[q, p], raw.at[q, p], got.at[p, q], {"group": to})

    def relay_given(p, q, to):
        return remote(raw.at[q, p, given], raw.at[q, p, given], got.at[p, q], {"group": to})

    whole = pl.ds(0, stage.shape[1])
    wide_part, rot_part = pl.ds(0, tail), pl.ds(tail, half)

    def rest(way, to):
        @pl.loop(2, seqs)
        def _(i):
            out(way, i, partner(c, i, seqs), whole, to).start()

    early = lower(c, seqs) + jnp.minimum(g, 1) + jnp.where(gate & (ens == 0), 1, 0)

    @pl.when(early > 0)
    def _():
        pl.semaphore_wait(barrier, early)

    @pl.when(below)
    def _():
        pl.semaphore_signal(ready.at[0], inc=1, device_id={"group": g - 1}, device_id_type=MESH)

    @pl.loop(0, c)
    def _(s):
        @pl.when(join(c, s, seqs) == c)
        def _():
            pl.semaphore_signal(ready.at[1 + c], inc=1, device_id={"ctx": s}, device_id_type=MESH)

    def prepare():
        for load in loads:
            load.wait()
        wide[...] = key_stage[...].astype(jnp.float32)
        for h in range(heads):
            key_w[h * key_part : (h + 1) * key_part, :] = (
                wide[pl.ds(h, latent, stride=heads), :].T.astype(BF16)
            )
        wide[...] = value_stage[...].astype(jnp.float32)
        for h in range(heads):
            value_w[:, h * size : (h + 1) * size] = (
                wide[pl.ds(h, latent, stride=heads), :].astype(BF16)
            )

    @pl.when(below & above)
    def _():
        for k in range(slabs):
            remote(
                lat.at[first, :, pl.ds(k * LANES, LANES)],
                mid.at[1 % ways, 0, 0, pl.ds(k * blk, blk)],
                mid_got.at[1 % ways, 0, 0], {"group": g - 1},
            ).start()

    for k in range(slabs):
        lat_load(first, k, 1).wait()

    @pl.loop(1, seqs)
    def _(b):
        for k in range(slabs):
            lat_load(partner(first, b, seqs), k, 0).wait()

    rot_load.wait()

    @pl.loop(0, seqs)
    def _(b):
        s = partner(first, b, seqs)
        block = rot_stage[s].astype(jnp.float32)
        both = jnp.concatenate([block[:half], block[half:]], axis=1)
        stage[s, pl.ds(tail, half), :] = both.astype(BF16)

    @pl.when(below & above)
    def _():
        out(1, 1, first, rot_part, g - 1).start()
        rest(1, g - 1)
        pl.when(jnp.logical_not(inner(1, 1)))(lambda: own_along(g - 1).start())
        pl.semaphore_wait(ready.at[0], 1)
        out(0, 1, first, whole, g + 1).start()
        rest(0, g + 1)
        pl.when(jnp.logical_not(inner(0, 1)))(lambda: own_along(g + 1).start())

    @pl.when(below & (g == planes - 1))
    def _():
        own_along(g - 1).start()

    @pl.when(above & (g == 0))
    def _():
        pl.semaphore_wait(ready.at[0], 1)
        own_along(g + 1).start()

    @pl.loop(c, seqs)
    def _(t):
        @pl.when(join(c, t, seqs) == t)
        def _():
            @pl.when(t > c)
            def _():
                pl.semaphore_wait(ready.at[1 + t], 1)

            @pl.loop(1, seqs)
            def _(i):
                s = partner(c, i, seqs)

                @pl.when(join(c, s, seqs) == t)
                def _():
                    own_side(s).start()

    raw[c, g] = stage[c]
    prepare()

    low = 2 * g < planes

    def near_first(go):
        pl.when(low)(lambda: go(1))
        go(0)
        pl.when(jnp.logical_not(low))(lambda: go(1))

    def arrived(p, q):
        relay(p, q, g).wait_recv()

    def plane(way, far):
        return g - far if way == 0 else g + far

    def exists(way, far):
        return g >= far if way == 0 else g + far < planes

    def onward(way):
        return above if way == 0 else below

    def towards(way):
        return g + 1 if way == 0 else g - 1

    def along(far):
        def go(way):
            @pl.when(exists(way, far))
            def _():
                arrived(plane(way, far), c)

                @pl.when(onward(way))
                def _():
                    relay(plane(way, far), c, towards(way)).start()

        near_first(go)

    def sized(way, go):
        if way == 0 or not give:
            go(whole)
        else:
            pl.when(c > 0)(lambda: go(whole))
            pl.when(c == 0)(lambda: go(kept))

    def pass_mid(far, i):
        def go(way):
            s = partner(c, i, seqs)

            @pl.when(inner(way, far))
            def _():
                if far == 1:
                    out(way, i, c, whole, g).wait_recv()
                    scatter(way, 0, i, whole, plane(way, far), s).start()

                    @pl.when(onward(way))
                    def _():
                        sized(way, lambda part: forward(way, i, part, towards(way)).start())
                else:
                    def onto(part):
                        forward(way, i, part, g).wait_recv()
                        scatter(way, 1, i, part, plane(way, far), s).start()

                    sized(way, onto)

        near_first(go)

    def take(far, i, chain=None):
        def go(way):
            wanted = exists(way, far)
            if chain is not None:
                wanted = wanted & (inner(way, far) != chain)

            @pl.when(wanted)
            def _():
                q = source(c, i, seqs)
                arrived(plane(way, far), q)

                @pl.when(onward(way) & ((far > 1) | jnp.logical_not(inner(way, 1))))
                def _():
                    relay(plane(way, far), q, towards(way)).start()

                if way == 1 and give:
                    @pl.when(below & inner(1, 1) & (far == 1) & (q == 0))
                    def _():
                        relay_given(plane(way, far), q, g - 1).start()

        near_first(go)

    end_q, end_u = pending(c, g, seqs, planes, units)

    def settle(q, low_far, high_far):
        @pl.loop(0, units)
        def _(u):
            far = jnp.maximum(g - u * per_unit, (u + 1) * per_unit - 1 - g)
            far = jnp.maximum(far, 1)
            wanted = (far >= low_far) & (far <= high_far)

            @pl.when(wanted & ((q != end_q) | (u != end_u)))
            def _():
                begin = u * per_unit
                start = pl.multiple_of((q * planes + begin) * blk, LANES)

                def block(row, count):
                    return raw[q, pl.ds(begin, per_unit), row : row + count, :]

                def put_keys(h, wide_keys, turned):
                    keys[h, :key_part, pl.ds(start, LANES)] = wide_keys
                    keys[h, key_part:, pl.ds(start, LANES)] = turned

                def put_values(rows):
                    at = pl.multiple_of(start * heads, LANES * heads)
                    values[pl.ds(at, LANES * heads), :] = rows

                expand(
                    block, slabs, blk, per_unit, heads, rotary, gain, key_w, value_w, mixed,
                    put_keys, put_values,
                )

    def own(i):
        q = source(c, i, seqs)
        arrived(g, q)

        @pl.when(above & (g == 0))
        def _():
            relay(g, q, g + 1).start()

        @pl.when(below & (g == planes - 1))
        def _():
            relay(g, q, g - 1).start()

    @pl.loop(1, seqs)
    def _(i):
        pl.when(g == planes - 1)(lambda: own(i))
        pl.when((g < planes - 1) | (g == 0))(lambda: pass_mid(1, i))
        pl.when((g == 0) & above)(lambda: own(i))

    @pl.loop(1, seqs)
    def _(i):
        pl.when((g == planes - 1) & below)(lambda: pass_mid(1, i))

    pl.when(inner(1, 1) & below)(lambda: own_along(g - 1).start())
    pl.when(inner(0, 1) & above)(lambda: own_along(g + 1).start())
    pl.when(jnp.logical_not(edge))(lambda: along(1))

    @pl.when(jnp.logical_not(edge))
    def _():
        settle(c, 1, 1)

        @pl.loop(1, seqs)
        def _(i):
            take(1, i, True)

    @pl.loop(1, seqs + 1)
    def _(i):
        @pl.when(i < seqs)
        def _():
            pass_mid(2, i)
            pl.when(jnp.logical_not(edge))(lambda: own(i))
            pl.when(edge)(lambda: take(1, i))
            pl.when(jnp.logical_not(edge))(lambda: take(1, i, False))

        @pl.when((i == seqs) & edge)
        def _():
            along(1)

        @pl.when((i < seqs) | edge)
        def _():
            settle(jnp.where(i == seqs, c, source(c, i, seqs)), 1, 1)

    along(2)

    def drain():
        ups, downs = jnp.minimum(planes - 1 - g, 1), jnp.minimum(g, 1)
        total = seqs * (ups + downs + g * ups + (planes - 1 - g) * downs)
        spread = sum(jnp.where(inner(way, far), 1, 0) for way in (0, 1) for far in (1, 2))
        total = total + (seqs - 1) * (1 + spread)
        near, next_near = jnp.where(inner(1, 1) & below, 1, 0), jnp.where(inner(1, 2), 1, 0)
        parts = jnp.where(c == 0, (seqs - 1) * (near + next_near), 0)
        if not give:
            parts = 0 * parts

        @pl.loop(0, total - parts)
        def _(_):
            own_along(g).wait_send()

        @pl.loop(0, parts)
        def _(_):
            forward(1, 1, kept, g).wait_send()

        if give:
            @pl.when((c > 0) & (near > 0))
            def _():
                relay_given(g, c, g).wait_send()

    pl.when(edge)(drain)

    def origin(i):
        return jnp.where(i == 0, c, source(c, jnp.maximum(i, 0), seqs))

    @pl.loop(2, max(planes, 3))
    def _(far):
        turn = gate & (far == planes - 2)

        @pl.loop(0, seqs + 1)
        def _(i):
            @pl.when((i == 0) & (far > 2))
            def _():
                along(far)

            @pl.when(turn & (ens == 1) & (i == max(seqs - HELD, 1)))
            def _():
                pl.semaphore_wait(ready.at[1], 1)

            at = jnp.where(edge, i, i - 1)
            late = turn & (ens == 1) & (i == seqs - 1) & (c == 0)
            pl.when(late)(lambda: settle(origin(at), far, far))

            @pl.when((i > 0) & (i < seqs))
            def _():
                take(far, i)

            done = turn & (ens == 0) & (i == seqs - 1)

            def release():
                pl.semaphore_signal(ready.at[1], inc=1, device_id={"ens": 1}, device_id_type=MESH)

            pl.when(done & (c > 0))(release)

            @pl.when((at >= 0) & (at < seqs) & jnp.logical_not(late))
            def _():
                settle(origin(at), far, far)

            pl.when(done & (c == 0))(release)

    last[...] = raw[end_q, pl.ds(end_u * per_unit, per_unit)]

    pl.when(jnp.logical_not(edge))(drain)


def store(
    seqs, planes, heads, rotary, blk,
    keys, values, last, key_w, value_w, gain,
    keys_out, values_out,
    end_keys, end_values, mixed, sems,
):
    c, g = lax.axis_index("ctx"), lax.axis_index("group")
    slabs = gain.shape[1] // LANES
    per_unit = LANES // blk
    units = planes // per_unit
    key_part = key_w.shape[0] // heads
    blocks = seqs * units
    end_q, end_u = pending(c, g, seqs, planes, units)
    end = end_q * units + end_u

    def columns(b):
        return pl.ds(pl.multiple_of(b * LANES, LANES), LANES)

    def rows(b):
        return pl.ds(pl.multiple_of(b * LANES * heads, LANES * heads), LANES * heads)

    @pl.loop(1, blocks)
    def _(j):
        b = lax.rem(end + j, blocks)
        pltpu.make_async_copy(
            keys.at[:, :, columns(b)], keys_out.at[:, :, columns(b)], sems.at[0]
        ).start()
        pltpu.make_async_copy(values.at[rows(b)], values_out.at[rows(b)], sems.at[1]).start()

    def block(row, count):
        return last[:, row : row + count, :]

    def put_keys(h, wide_keys, turned):
        end_keys[h, :key_part, :] = wide_keys
        end_keys[h, key_part:, :] = turned

    def put_values(part):
        end_values[...] = part

    expand(
        block, slabs, blk, per_unit, heads, rotary, gain, key_w, value_w, mixed,
        put_keys, put_values,
    )
    pltpu.make_async_copy(end_keys, keys_out.at[:, :, columns(end)], sems.at[0]).start()
    pltpu.make_async_copy(end_values, values_out.at[rows(end)], sems.at[1]).start()
    pltpu.make_async_copy(keys, keys_out, sems.at[0]).wait()
    pltpu.make_async_copy(values, values_out, sems.at[1]).wait()


def per_device(latents, rotary_rows, latent_gain, key_up, value_up):
    seqs, planes = lax.axis_size("ctx"), lax.axis_size("group")
    _, blk, latent = latents.shape
    rotary = rotary_rows.shape[2]
    heads, key_part = key_up.shape[1:]
    size = value_up.shape[2]
    length = seqs * planes * blk
    per_unit = LANES // blk
    ways = 1 if planes <= 4 else 2
    packed = (blk * (latent + rotary) // LANES, LANES)
    dma = pltpu.SemaphoreType.DMA
    in_hbm = functools.partial(pltpu.with_memory_space_constraint, memory_space=pltpu.HBM)
    outer = pl.BlockSpec(memory_space=pltpu.HBM)
    inside = pl.BlockSpec(memory_space=pltpu.VMEM)
    held = pl.pallas_call(
        functools.partial(kernel, seqs, planes, heads, rotary),
        out_shape=(
            pltpu.VMEM((heads, key_part + rotary, length), BF16),
            pltpu.VMEM((length * heads, size), BF16),
            pltpu.VMEM((per_unit, *packed), BF16),
            pltpu.VMEM((heads * key_part, latent), BF16),
            pltpu.VMEM((latent, heads * size), BF16),
            pltpu.VMEM((1, latent), jnp.float32),
        ),
        in_specs=[outer] * 5,
        out_specs=(inside,) * 6,
        scratch_shapes=[
            pltpu.VMEM((seqs, *packed), BF16),
            pltpu.VMEM((seqs, planes, *packed), BF16),
            pltpu.VMEM((ways, 2, seqs - 1, *packed), BF16),
            pltpu.VMEM((seqs, blk, rotary), BF16),
            pltpu.VMEM((latent * heads, key_part), BF16),
            pltpu.VMEM((latent * heads, size), BF16),
            pltpu.VMEM((latent * heads, size), jnp.float32),
            pltpu.VMEM((LANES * heads, size), jnp.float32),
            dma((3,)),
            dma((planes, seqs)),
            dma((ways, 2, seqs - 1)),
            dma,
            pltpu.SemaphoreType.REGULAR((1 + seqs,)),
        ],
        compiler_params=pltpu.CompilerParams(
            collective_id=0, has_side_effects=True, vmem_limit_bytes=32 * 1024 * 1024
        ),
    )(
        in_hbm(latents),
        in_hbm(rotary_rows),
        in_hbm(latent_gain.reshape(1, latent)),
        in_hbm(key_up.reshape(latent * heads, key_part)),
        in_hbm(value_up.reshape(latent * heads, size)),
    )
    keys, values = pl.pallas_call(
        functools.partial(store, seqs, planes, heads, rotary, blk),
        out_shape=(
            jax.ShapeDtypeStruct((heads, key_part + rotary, length), BF16),
            jax.ShapeDtypeStruct((length * heads, size), BF16),
        ),
        in_specs=[inside] * 6,
        out_specs=(outer, outer),
        scratch_shapes=[
            pltpu.VMEM((heads, key_part + rotary, LANES), BF16),
            pltpu.VMEM((LANES * heads, size), BF16),
            pltpu.VMEM((LANES * heads, size), jnp.float32),
            dma((2,)),
        ],
        compiler_params=pltpu.CompilerParams(vmem_limit_bytes=16 * 1024 * 1024),
    )(*held)
    return keys[None], values.reshape(1, length, heads, size)


def solution(mesh):
    in_specs = (
        P("ens", ("ctx", "group"), None),
        P("ens", ("ctx", "group"), None),
        P(),
        P("ens", "group", None),
        P("ens", "group", None),
    )
    out_specs = (P(("ens", "ctx"), "group", None, None), P(("ens", "ctx"), None, "group", None))
    return jax.shard_map(
        per_device, mesh=mesh, in_specs=in_specs, out_specs=out_specs, check_vma=False
    )
```

```python
import functools

import jax
import jax.numpy as jnp
from jax import lax
from jax.experimental import pallas as pl
from jax.experimental.pallas import tpu as pltpu
from jax.sharding import PartitionSpec as P

MESH = pl.DeviceIdType.MESH
LANES = 128
BF16 = jnp.bfloat16
GIVEN = 2, 18
HELD = 1


def xor(me, step, count):
    total, bit = 0, 1
    while bit < count:
        total = total + bit * lax.rem(me // bit + step // bit, 2)
        bit *= 2
    return total


def partner(me, step, count):
    return lax.rem(me + step, count) if count & (count - 1) else xor(me, step, count)


def source(me, step, count):
    return lax.rem(me + count - step, count) if count & (count - 1) else xor(me, step, count)


def join(a, b, count):
    if count & (count - 1):
        return jnp.maximum(a, b)
    total, bit = 0, 1
    while bit < count:
        total = total + bit * jnp.maximum(lax.rem(a // bit, 2), lax.rem(b // bit, 2))
        bit *= 2
    return total


def lower(c, count):
    if count & (count - 1):
        return c
    total, bit = 1, 1
    while bit < count:
        total = total * (1 + lax.rem(c // bit, 2))
        bit *= 2
    return total - 1


def pending(c, g, seqs, planes, units):
    q = source(c, seqs - 1, seqs) if seqs > 1 else c
    return q, jnp.where(2 * g < planes, units - 1, 0)


def expand(block, slabs, blk, per_unit, heads, rotary, gain, key_w, value_w, mixed, put_keys, put_values):
    key_part = key_w.shape[0] // heads
    size = value_w.shape[1] // heads
    x = jnp.concatenate(
        [block(k * blk, blk).astype(jnp.float32).reshape(LANES, LANES) for k in range(slabs)],
        axis=1,
    )
    mean = jnp.mean(x * x, axis=-1, keepdims=True)
    rows = (x * lax.rsqrt(mean + 1e-06) * gain[...]).astype(BF16)
    wide_keys = lax.dot_general(
        key_w[...], rows, (((1,), (1,)), ((), ())), preferred_element_type=jnp.float32
    ).astype(BF16)
    tails = block(slabs * blk, blk * rotary // LANES).astype(jnp.float32)
    pieces = []
    for j in range(per_unit):
        pieces += [tails[j][:, :rotary], pltpu.roll(tails[j], rotary, 1)[:, :rotary]]
    turned = jnp.concatenate(pieces, axis=0).T.astype(BF16)
    for h in range(heads):
        put_keys(h, wide_keys[h * key_part : (h + 1) * key_part], turned)
    wide_values = jnp.dot(rows, value_w[...], preferred_element_type=jnp.float32)
    for h in range(heads):
        mixed[pl.ds(h, LANES, stride=heads), :] = wide_values[:, h * size : (h + 1) * size]
    put_values(mixed[...].astype(BF16))


def kernel(
    seqs, planes, heads, rotary,
    lat, rot, gain_in, key_up, value_up,
    keys, values, last, key_w, value_w, gain,
    stage, raw, mid, rot_stage, key_stage, value_stage, wide, mixed,
    load_sem, got, mid_got, sent, ready,
):
    ens, c, g = lax.axis_index("ens"), lax.axis_index("ctx"), lax.axis_index("group")
    blk, latent = lat.shape[1:]
    slabs = latent // LANES
    tail = slabs * blk
    half = blk // 2
    give = stage.shape[1] // 16 * GIVEN[0] // GIVEN[1] * 16
    keep = stage.shape[1] - give
    kept, given = pl.ds(0, keep), pl.ds(keep, give)
    ways = mid.shape[0]
    per_unit = LANES // blk
    units = planes // per_unit
    key_part = key_w.shape[0] // heads
    size = value_w.shape[1] // heads
    first = partner(c, 1, seqs)

    def lat_load(s, k, sem):
        return pltpu.make_async_copy(
            lat.at[s, :, pl.ds(k * LANES, LANES)],
            stage.at[s, pl.ds(k * blk, blk), :],
            load_sem.at[sem],
        )

    rot_load = pltpu.make_async_copy(rot, rot_stage, load_sem.at[0])
    for k in range(slabs):
        lat_load(first, k, 1).start()
    rot_load.start()

    barrier = pltpu.get_barrier_semaphore()
    above, below = g < planes - 1, g > 0
    edge = (g == 0) | (g == planes - 1)
    gate = (g == 1) | (g == planes - 2) if planes > 3 else g < 0

    def inner(way, far):
        return g > far if way == 0 else g + far < planes - 1

    @pl.when(above)
    def _():
        pl.semaphore_signal(barrier, inc=1, device_id={"group": g + 1}, device_id_type=MESH)

    @pl.when(gate & (ens == 1))
    def _():
        pl.semaphore_signal(barrier, inc=1, device_id={"ens": 0}, device_id_type=MESH)

    @pl.loop(c + 1, seqs)
    def _(s):
        @pl.when(join(c, s, seqs) == s)
        def _():
            pl.semaphore_signal(barrier, inc=1, device_id={"ctx": s}, device_id_type=MESH)

    def remote(src, dst, in_sem, to):
        return pltpu.make_async_remote_copy(
            src_ref=src, dst_ref=dst, send_sem=sent, recv_sem=in_sem,
            device_id=to, device_id_type=MESH,
        )

    def out(way, i, s, part, to):
        return remote(
            stage.at[s, part], mid.at[way % ways, 0, i - 1, part], mid_got.at[way % ways, 0, i - 1], {"group": to}
        )

    def own_along(to):
        return remote(stage.at[c], raw.at[c, g], got.at[g, c], {"group": to})

    def own_side(s):
        return remote(stage.at[s], raw.at[c, g], got.at[g, c], {"ctx": s})

    def forward(way, i, part, to):
        return remote(
            mid.at[way % ways, 0, i - 1, part], mid.at[way % ways, 1, i - 1, part],
            mid_got.at[way % ways, 1, i - 1], {"group": to},
        )

    def scatter(way, far, i, part, p, s):
        return remote(mid.at[way % ways, far, i - 1, part], raw.at[c, p, part], got.at[p, c], {"ctx": s})

    def relay(p, q, to):
        return remote(raw.at[q, p], raw.at[q, p], got.at[p, q], {"group": to})

    def relay_given(p, q, to):
        return remote(raw.at[q, p, given], raw.at[q, p, given], got.at[p, q], {"group": to})

    whole = pl.ds(0, stage.shape[1])
    wide_part, rot_part = pl.ds(0, tail), pl.ds(tail, half)

    def rest(way, to):
        @pl.loop(2, seqs)
        def _(i):
            out(way, i, partner(c, i, seqs), whole, to).start()

    @pl.loop(1, seqs)
    def _(b):
        for k in range(slabs):
            lat_load(partner(first, b, seqs), k, 0).start()

    loads = [
        pltpu.make_async_copy(key_up, key_stage, load_sem.at[2]),
        pltpu.make_async_copy(value_up, value_stage, load_sem.at[2]),
        pltpu.make_async_copy(gain_in, gain, load_sem.at[2]),
    ]
    for load in loads:
        load.start()

    early = lower(c, seqs) + jnp.minimum(g, 1) + jnp.where(gate & (ens == 0), 1, 0)

    @pl.when(early > 0)
    def _():
        pl.semaphore_wait(barrier, early)

    @pl.when(below)
    def _():
        pl.semaphore_signal(ready.at[0], inc=1, device_id={"group": g - 1}, device_id_type=MESH)

    @pl.loop(0, c)
    def _(s):
        @pl.when(join(c, s, seqs) == c)
        def _():
            pl.semaphore_signal(ready.at[1 + c], inc=1, device_id={"ctx": s}, device_id_type=MESH)

    def prepare():
        for load in loads:
            load.wait()
        wide[...] = key_stage[...].astype(jnp.float32)
        for h in range(heads):
            key_w[h * key_part : (h + 1) * key_part, :] = (
                wide[pl.ds(h, latent, stride=heads), :].T.astype(BF16)
            )
        wide[...] = value_stage[...].astype(jnp.float32)
        for h in range(heads):
            value_w[:, h * size : (h + 1) * size] = (
                wide[pl.ds(h, latent, stride=heads), :].astype(BF16)
            )

    @pl.when(below & above)
    def _():
        for k in range(slabs):
            remote(
                lat.at[first, :, pl.ds(k * LANES, LANES)],
                mid.at[1 % ways, 0, 0, pl.ds(k * blk, blk)],
                mid_got.at[1 % ways, 0, 0], {"group": g - 1},
            ).start()

    for k in range(slabs):
        lat_load(first, k, 1).wait()

    @pl.loop(1, seqs)
    def _(b):
        for k in range(slabs):
            lat_load(partner(first, b, seqs), k, 0).wait()

    rot_load.wait()

    @pl.loop(0, seqs)
    def _(b):
        s = partner(first, b, seqs)
        block = rot_stage[s].astype(jnp.float32)
        both = jnp.concatenate([block[:half], block[half:]], axis=1)
        stage[s, pl.ds(tail, half), :] = both.astype(BF16)

    @pl.when(below & above)
    def _():
        out(1, 1, first, rot_part, g - 1).start()
        rest(1, g - 1)
        pl.when(jnp.logical_not(inner(1, 1)))(lambda: own_along(g - 1).start())
        pl.semaphore_wait(ready.at[0], 1)
        out(0, 1, first, whole, g + 1).start()
        rest(0, g + 1)
        pl.when(jnp.logical_not(inner(0, 1)))(lambda: own_along(g + 1).start())

    @pl.when(below & (g == planes - 1))
    def _():
        own_along(g - 1).start()

    @pl.when(above & (g == 0))
    def _():
        pl.semaphore_wait(ready.at[0], 1)
        own_along(g + 1).start()

    @pl.loop(c, seqs)
    def _(t):
        @pl.when(join(c, t, seqs) == t)
        def _():
            @pl.when(t > c)
            def _():
                pl.semaphore_wait(ready.at[1 + t], 1)

            @pl.loop(1, seqs)
            def _(i):
                s = partner(c, i, seqs)

                @pl.when(join(c, s, seqs) == t)
                def _():
                    own_side(s).start()

    raw[c, g] = stage[c]
    prepare()

    low = 2 * g < planes

    def near_first(go):
        pl.when(low)(lambda: go(1))
        go(0)
        pl.when(jnp.logical_not(low))(lambda: go(1))

    def arrived(p, q):
        relay(p, q, g).wait_recv()

    def plane(way, far):
        return g - far if way == 0 else g + far

    def exists(way, far):
        return g >= far if way == 0 else g + far < planes

    def onward(way):
        return above if way == 0 else below

    def towards(way):
        return g + 1 if way == 0 else g - 1

    def along(far):
        def go(way):
            @pl.when(exists(way, far))
            def _():
                arrived(plane(way, far), c)

                @pl.when(onward(way))
                def _():
                    relay(plane(way, far), c, towards(way)).start()

        near_first(go)

    def sized(way, go):
        if way == 0 or not give:
            go(whole)
        else:
            pl.when(c > 0)(lambda: go(whole))
            pl.when(c == 0)(lambda: go(kept))

    def pass_mid(far, i):
        def go(way):
            s = partner(c, i, seqs)

            @pl.when(inner(way, far))
            def _():
                if far == 1:
                    out(way, i, c, whole, g).wait_recv()
                    scatter(way, 0, i, whole, plane(way, far), s).start()

                    @pl.when(onward(way))
                    def _():
                        sized(way, lambda part: forward(way, i, part, towards(way)).start())
                else:
                    def onto(part):
                        forward(way, i, part, g).wait_recv()
                        scatter(way, 1, i, part, plane(way, far), s).start()

                    sized(way, onto)

        near_first(go)

    def take(far, i, chain=None):
        def go(way):
            wanted = exists(way, far)
            if chain is not None:
                wanted = wanted & (inner(way, far) != chain)

            @pl.when(wanted)
            def _():
                q = source(c, i, seqs)
                arrived(plane(way, far), q)

                @pl.when(onward(way) & ((far > 1) | jnp.logical_not(inner(way, 1))))
                def _():
                    relay(plane(way, far), q, towards(way)).start()

                if way == 1 and give:
                    @pl.when(below & inner(1, 1) & (far == 1) & (q == 0))
                    def _():
                        relay_given(plane(way, far), q, g - 1).start()

        near_first(go)

    end_q, end_u = pending(c, g, seqs, planes, units)

    def settle(q, low_far, high_far):
        @pl.loop(0, units)
        def _(u):
            far = jnp.maximum(g - u * per_unit, (u + 1) * per_unit - 1 - g)
            far = jnp.maximum(far, 1)
            wanted = (far >= low_far) & (far <= high_far)

            @pl.when(wanted & ((q != end_q) | (u != end_u)))
            def _():
                begin = u * per_unit
                start = pl.multiple_of((q * planes + begin) * blk, LANES)

                def block(row, count):
                    return raw[q, pl.ds(begin, per_unit), row : row + count, :]

                def put_keys(h, wide_keys, turned):
                    keys[h, :key_part, pl.ds(start, LANES)] = wide_keys
                    keys[h, key_part:, pl.ds(start, LANES)] = turned

                def put_values(rows):
                    at = pl.multiple_of(start * heads, LANES * heads)
                    values[pl.ds(at, LANES * heads), :] = rows

                expand(
                    block, slabs, blk, per_unit, heads, rotary, gain, key_w, value_w, mixed,
                    put_keys, put_values,
                )

    def own(i):
        q = source(c, i, seqs)
        arrived(g, q)

        @pl.when(above & (g == 0))
        def _():
            relay(g, q, g + 1).start()

        @pl.when(below & (g == planes - 1))
        def _():
            relay(g, q, g - 1).start()

    @pl.loop(1, seqs)
    def _(i):
        pl.when(g == planes - 1)(lambda: own(i))
        pl.when((g < planes - 1) | (g == 0))(lambda: pass_mid(1, i))
        pl.when((g == 0) & above)(lambda: own(i))

    @pl.loop(1, seqs)
    def _(i):
        pl.when((g == planes - 1) & below)(lambda: pass_mid(1, i))

    pl.when(inner(1, 1) & below)(lambda: own_along(g - 1).start())
    pl.when(inner(0, 1) & above)(lambda: own_along(g + 1).start())
    pl.when(jnp.logical_not(edge))(lambda: along(1))

    @pl.when(jnp.logical_not(edge))
    def _():
        settle(c, 1, 1)

        @pl.loop(1, seqs)
        def _(i):
            take(1, i, True)

    @pl.loop(1, seqs + 1)
    def _(i):
        @pl.when(i < seqs)
        def _():
            pass_mid(2, i)
            pl.when(jnp.logical_not(edge))(lambda: own(i))
            pl.when(edge)(lambda: take(1, i))
            pl.when(jnp.logical_not(edge))(lambda: take(1, i, False))

        @pl.when((i == seqs) & edge)
        def _():
            along(1)

        @pl.when((i < seqs) | edge)
        def _():
            settle(jnp.where(i == seqs, c, source(c, i, seqs)), 1, 1)

    along(2)

    def drain():
        ups, downs = jnp.minimum(planes - 1 - g, 1), jnp.minimum(g, 1)
        total = seqs * (ups + downs + g * ups + (planes - 1 - g) * downs)
        spread = sum(jnp.where(inner(way, far), 1, 0) for way in (0, 1) for far in (1, 2))
        total = total + (seqs - 1) * (1 + spread)
        near, next_near = jnp.where(inner(1, 1) & below, 1, 0), jnp.where(inner(1, 2), 1, 0)
        parts = jnp.where(c == 0, (seqs - 1) * (near + next_near), 0)
        if not give:
            parts = 0 * parts

        @pl.loop(0, total - parts)
        def _(_):
            own_along(g).wait_send()

        @pl.loop(0, parts)
        def _(_):
            forward(1, 1, kept, g).wait_send()

        if give:
            @pl.when((c > 0) & (near > 0))
            def _():
                relay_given(g, c, g).wait_send()

    pl.when(edge)(drain)

    def origin(i):
        return jnp.where(i == 0, c, source(c, jnp.maximum(i, 0), seqs))

    @pl.loop(2, max(planes, 3))
    def _(far):
        turn = gate & (far == planes - 2)

        @pl.loop(0, seqs + 1)
        def _(i):
            @pl.when((i == 0) & (far > 2))
            def _():
                along(far)

            @pl.when(turn & (ens == 1) & (i == max(seqs - HELD, 1)))
            def _():
                pl.semaphore_wait(ready.at[1], 1)

            at = jnp.where(edge, i, i - 1)
            late = turn & (ens == 1) & (i == seqs - 1) & (c == 0)
            pl.when(late)(lambda: settle(origin(at), far, far))

            @pl.when((i > 0) & (i < seqs))
            def _():
                take(far, i)

            done = turn & (ens == 0) & (i == seqs - 1)

            def release():
                pl.semaphore_signal(ready.at[1], inc=1, device_id={"ens": 1}, device_id_type=MESH)

            pl.when(done & (c > 0))(release)

            @pl.when((at >= 0) & (at < seqs) & jnp.logical_not(late))
            def _():
                settle(origin(at), far, far)

            pl.when(done & (c == 0))(release)

    last[...] = raw[end_q, pl.ds(end_u * per_unit, per_unit)]

    pl.when(jnp.logical_not(edge))(drain)


def store(
    seqs, planes, heads, rotary, blk,
    keys, values, last, key_w, value_w, gain,
    keys_out, values_out,
    end_keys, end_values, mixed, sems,
):
    c, g = lax.axis_index("ctx"), lax.axis_index("group")
    slabs = gain.shape[1] // LANES
    per_unit = LANES // blk
    units = planes // per_unit
    key_part = key_w.shape[0] // heads
    blocks = seqs * units
    end_q, end_u = pending(c, g, seqs, planes, units)
    end = end_q * units + end_u

    def columns(b):
        return pl.ds(pl.multiple_of(b * LANES, LANES), LANES)

    def rows(b):
        return pl.ds(pl.multiple_of(b * LANES * heads, LANES * heads), LANES * heads)

    @pl.loop(1, blocks)
    def _(j):
        b = lax.rem(end + j, blocks)
        pltpu.make_async_copy(
            keys.at[:, :, columns(b)], keys_out.at[:, :, columns(b)], sems.at[0]
        ).start()
        pltpu.make_async_copy(values.at[rows(b)], values_out.at[rows(b)], sems.at[1]).start()

    def block(row, count):
        return last[:, row : row + count, :]

    def put_keys(h, wide_keys, turned):
        end_keys[h, :key_part, :] = wide_keys
        end_keys[h, key_part:, :] = turned

    def put_values(part):
        end_values[...] = part

    expand(
        block, slabs, blk, per_unit, heads, rotary, gain, key_w, value_w, mixed,
        put_keys, put_values,
    )
    pltpu.make_async_copy(end_keys, keys_out.at[:, :, columns(end)], sems.at[0]).start()
    pltpu.make_async_copy(end_values, values_out.at[rows(end)], sems.at[1]).start()
    pltpu.make_async_copy(keys, keys_out, sems.at[0]).wait()
    pltpu.make_async_copy(values, values_out, sems.at[1]).wait()


def per_device(latents, rotary_rows, latent_gain, key_up, value_up):
    seqs, planes = lax.axis_size("ctx"), lax.axis_size("group")
    _, blk, latent = latents.shape
    rotary = rotary_rows.shape[2]
    heads, key_part = key_up.shape[1:]
    size = value_up.shape[2]
    length = seqs * planes * blk
    per_unit = LANES // blk
    ways = 1 if planes <= 4 else 2
    packed = (blk * (latent + rotary) // LANES, LANES)
    dma = pltpu.SemaphoreType.DMA
    in_hbm = functools.partial(pltpu.with_memory_space_constraint, memory_space=pltpu.HBM)
    outer = pl.BlockSpec(memory_space=pltpu.HBM)
    inside = pl.BlockSpec(memory_space=pltpu.VMEM)
    held = pl.pallas_call(
        functools.partial(kernel, seqs, planes, heads, rotary),
        out_shape=(
            pltpu.VMEM((heads, key_part + rotary, length), BF16),
            pltpu.VMEM((length * heads, size), BF16),
            pltpu.VMEM((per_unit, *packed), BF16),
            pltpu.VMEM((heads * key_part, latent), BF16),
            pltpu.VMEM((latent, heads * size), BF16),
            pltpu.VMEM((1, latent), jnp.float32),
        ),
        in_specs=[outer] * 5,
        out_specs=(inside,) * 6,
        scratch_shapes=[
            pltpu.VMEM((seqs, *packed), BF16),
            pltpu.VMEM((seqs, planes, *packed), BF16),
            pltpu.VMEM((ways, 2, seqs - 1, *packed), BF16),
            pltpu.VMEM((seqs, blk, rotary), BF16),
            pltpu.VMEM((latent * heads, key_part), BF16),
            pltpu.VMEM((latent * heads, size), BF16),
            pltpu.VMEM((latent * heads, size), jnp.float32),
            pltpu.VMEM((LANES * heads, size), jnp.float32),
            dma((3,)),
            dma((planes, seqs)),
            dma((ways, 2, seqs - 1)),
            dma,
            pltpu.SemaphoreType.REGULAR((1 + seqs,)),
        ],
        compiler_params=pltpu.CompilerParams(
            collective_id=0, has_side_effects=True, vmem_limit_bytes=32 * 1024 * 1024
        ),
    )(
        in_hbm(latents),
        in_hbm(rotary_rows),
        in_hbm(latent_gain.reshape(1, latent)),
        in_hbm(key_up.reshape(latent * heads, key_part)),
        in_hbm(value_up.reshape(latent * heads, size)),
    )
    keys, values = pl.pallas_call(
        functools.partial(store, seqs, planes, heads, rotary, blk),
        out_shape=(
            jax.ShapeDtypeStruct((heads, key_part + rotary, length), BF16),
            jax.ShapeDtypeStruct((length * heads, size), BF16),
        ),
        in_specs=[inside] * 6,
        out_specs=(outer, outer),
        scratch_shapes=[
            pltpu.VMEM((heads, key_part + rotary, LANES), BF16),
            pltpu.VMEM((LANES * heads, size), BF16),
            pltpu.VMEM((LANES * heads, size), jnp.float32),
            dma((2,)),
        ],
        compiler_params=pltpu.CompilerParams(vmem_limit_bytes=16 * 1024 * 1024),
    )(*held)
    return keys[None], values.reshape(1, length, heads, size)


def solution(mesh):
    in_specs = (
        P("ens", ("ctx", "group"), None),
        P("ens", ("ctx", "group"), None),
        P(),
        P("ens", "group", None),
        P("ens", "group", None),
    )
    out_specs = (P(("ens", "ctx"), "group", None, None), P(("ens", "ctx"), None, "group", None))
    return jax.shard_map(
        per_device, mesh=mesh, in_specs=in_specs, out_specs=out_specs, check_vma=False
    )
```
